512 devices in a mesh: ia: 8 (over x, z_hi), ja: 8 (over z_lo), ka: 8 (over y, core).
Axes of the slice: x: 4, y: 4, z: 16 (z_hi: 2, z_lo: 8; z = z_hi * 8 + z_lo), core: 2. Of those that a mesh axis runs over, the one named last changes fastest.
Arguments:
- tensor: bfloat16 [512, 512, 2, 1024], P('ia', 'ja', None, 'ka'), may hold values from -6 to 6
- factor_two: float32 [512, 32], P('ja'), may hold values from -2 to 2
- factor_three: float32 [1024, 32], P('ka'), may hold values from -2 to 2
- factor_four: float32 [2, 32], replicated, may hold values from -2 to 2
Outputs:
- new_one: float32 [512, 32], P('ia')
- new_two: float32 [512, 32], P('ja')
The draws below stay inside these ranges and needn't reach their ends.
All inputs are finite; a program needn't handle non-finite values.
Results may differ from the reference program's by a relative error of at most 0.0042.
Values sent between devices are 32-bit elements; how exact they have to be, the bound alone decides.
No kernel may reach another device: no remote copies, remote signals or barrier semaphores. Data moves between devices by JAX's collectives and lax.ppermute only.
A program may use at most 64 MiB of HBM per device.

```python
import math
import jax
import jax.numpy as jnp
from jax import lax

RANK = 32
FOURTH = 2
DIM_ONE = 512
DIM_TWO = 512
DIM_THREE = 1024


def loguniform_draw(key, extent, lowest, highest):
    return jnp.exp(jax.random.uniform(key, extent, jnp.float32, math.log(lowest), math.log(highest)))


def log_mean_square(lowest, highest):
    return (highest * highest - lowest * lowest) / (2.0 * math.log(highest / lowest))


def correlated_factor(key, row_count):
    subkeys = jax.random.split(key, 4)
    common_weight = 1.2
    column_lowest = 0.6
    column_highest = 1.4
    row_lowest = 0.3
    row_highest = 3.0
    noise = jax.random.truncated_normal(subkeys[0], -3.0, 3.0, (row_count, RANK), jnp.float32)
    common = jax.random.truncated_normal(subkeys[1], -3.0, 3.0, (row_count, 1), jnp.float32)
    column = loguniform_draw(subkeys[2], (1, RANK), column_lowest, column_highest)
    row_scale = loguniform_draw(subkeys[3], (row_count, 1), row_lowest, row_highest)
    spread = log_mean_square(row_lowest, row_highest) * (1.0 + common_weight * common_weight * log_mean_square(column_lowest, column_highest))
    return row_scale * (noise + common_weight * common * column) / math.sqrt(row_count * spread)


def draw_factor_two(key, part):
    return correlated_factor(jax.random.fold_in(key, 21), DIM_TWO)


def draw_factor_three(key, part):
    return correlated_factor(jax.random.fold_in(key, 22), DIM_THREE)


def draw_factor_four(key, part):
    subkeys = jax.random.split(jax.random.fold_in(key, 23), 2)
    signs = (2 * jax.random.randint(subkeys[0], (FOURTH, 1), 0, 2) - 1).astype(jnp.float32)
    magnitude = jax.random.uniform(subkeys[1], (FOURTH, RANK), jnp.float32, 0.5, 1.5)
    return signs * magnitude / math.sqrt(FOURTH)


def level_of(rng, shape, pieces, least, top_value):
    level = 1.0
    for dim, parts in pieces:
        draws = jax.random.uniform(jax.random.fold_in(jax.random.fold_in(rng, 6), dim), (parts,), jnp.float32, least / len(pieces), top_value / len(pieces))
        level = level * jnp.repeat(jnp.exp(draws), shape[dim] // parts).reshape((-1,) + (1,) * (len(shape) - 1 - dim))
    return level


def gaussian(key, dims, scale, reach, cuts=(), dtype=jnp.bfloat16):
    values = scale * jax.random.normal(key, dims, jnp.float32)
    if cuts:
        values = values * level_of(key, dims, cuts, -0.22, 0.18)
    return jnp.clip(values, -reach, reach).astype(dtype)


def setup_inputs(seed: int = 0) -> dict:
    arg_keys = jax.random.split(jax.random.key(seed), 5)
    tensor = gaussian(arg_keys[0], (DIM_ONE, DIM_TWO, FOURTH, DIM_THREE), 1.0, 6.0, ((0, 8), (1, 8), (3, 8)))
    factor_two = draw_factor_two(jax.random.fold_in(arg_keys[4], 71), 0)
    factor_three = draw_factor_three(jax.random.fold_in(arg_keys[4], 71), 0)
    factor_four = draw_factor_four(jax.random.fold_in(arg_keys[4], 71), 0)
    return {"tensor": tensor, "factor_two": factor_two, "factor_three": factor_three, "factor_four": factor_four}


def solve_rows(rhs, system):
    lower = jnp.linalg.cholesky(system)
    return jax.scipy.linalg.cho_solve((lower, True), rhs.T).T

def gram(factor):
    return jnp.dot(factor.T, factor, precision=lax.Precision.HIGHEST)

def reference(tensor, factor_two, factor_three, factor_four):
    khatri = (factor_four[:, None, :] * factor_three[None, :, :]).reshape(FOURTH * DIM_THREE, RANK).astype(jnp.bfloat16)
    flat = tensor.reshape(DIM_ONE, DIM_TWO, FOURTH * DIM_THREE)
    root = lax.map(lambda slab: jnp.dot(slab.astype(jnp.float32), khatri.astype(jnp.float32), preferred_element_type=jnp.float32), flat)
    gram_two = gram(factor_two)
    gram_three = gram(factor_three)
    gram_four = gram(factor_four)
    mode_one = jnp.einsum('abr,br->ar', root, factor_two, precision=lax.Precision.HIGHEST)
    new_one = solve_rows(mode_one, gram_two * gram_three * gram_four)
    gram_one = gram(new_one)
    mode_two = jnp.einsum('abr,ar->br', root, new_one, precision=lax.Precision.HIGHEST)
    new_two = solve_rows(mode_two, gram_one * gram_three * gram_four)
    return (new_one, new_two)
```

```python
import functools

import jax
import jax.numpy as jnp
from jax import lax
from jax.experimental import pallas as pl
from jax.experimental.pallas import tpu as pltpu
from jax.sharding import PartitionSpec as P

HI = lax.Precision.HIGHEST
LANES = 128
SUB = 8
VMEM = pl.BlockSpec(memory_space=pltpu.VMEM)
PARAMS = pltpu.CompilerParams(vmem_limit_bytes=24 * 1024 * 1024)


def iota(shape, dim):
    return lax.broadcasted_iota(jnp.int32, shape, dim)


def contract_last(a, b, precision=HI):
    return lax.dot_general(
        a, b, (((1,), (1,)), ((), ())), precision=precision, preferred_element_type=jnp.float32
    )


def fold_matrix(rank, fourth):
    shape = (rank, fourth * rank)
    return (iota(shape, 1) % rank == iota(shape, 0)).astype(jnp.float32)


def fill_slots(out_ref, value):
    for slot in range(out_ref.shape[0]):
        out_ref[slot] = value


def summed_slots(ref):
    parts = [ref[s] for s in range(ref.shape[0])]
    while len(parts) > 1:
        parts = [a + b for a, b in zip(parts[::2], parts[1::2])]
    return parts[0]


def root_kernel(first, chunks, x_hbm, f2t_ref, f3t_ref, f4_ref, prod_ref, pay_ref, x_ref, r_ref, sems):
    fourth, rank = f4_ref.shape
    second = f2t_ref.shape[1]
    wide = fourth * rank
    rows = second * fourth
    per = first // chunks
    span = per * rows

    def fetch(c):
        part = pl.ds(c * span, span)
        return pltpu.make_async_copy(x_hbm.at[part], x_ref.at[part], sems.at[c])

    for c in range(chunks):
        fetch(c).start()

    f2t = f2t_ref[...]
    f3t = f3t_ref[...]
    f4 = f4_ref[...]
    eye = iota((rank, rank), 0) == iota((rank, rank), 1)
    cols = [
        jnp.sum(jnp.where(eye, f4[l : l + 1, :], 0.0), axis=1, keepdims=True) for l in range(fourth)
    ]
    kt = jnp.concatenate([c * f3t for c in cols], axis=0).astype(jnp.bfloat16)

    gram_four = sum(cols[l] * f4[l : l + 1, :] for l in range(fourth))
    gram_two = contract_last(f2t, f2t)
    gram_rest = contract_last(f3t, f3t) * gram_four
    grams = jnp.concatenate(
        [jnp.zeros((rank, LANES - 2 * rank), jnp.float32), gram_two, gram_rest * 0.125], axis=1
    )

    spread = (iota((rows, second), 0) // fourth == iota((rows, second), 1)).astype(jnp.float32)
    weight = contract_last(spread, jnp.concatenate([f2t] * fourth, axis=0))
    keep = iota((rows, wide), 0) % fourth == iota((rows, wide), 1) // rank
    weight = jnp.where(keep, weight, 0.0).reshape(1, rows // SUB, SUB, wide)

    for c in range(chunks):
        fetch(c).wait()
        part = contract_last(x_ref[pl.ds(c * span, span), :], kt, None)
        prod_ref[pl.ds(c * span, span), :] = part
        r_ref[pl.ds(c * per * SUB, per * SUB), :] = jnp.sum(
            part.reshape(per, rows // SUB, SUB, wide) * weight, axis=1
        ).reshape(per * SUB, wide)

    total = r_ref[pl.ds(0, first, stride=SUB), :]
    for s in range(1, SUB):
        total = total + r_ref[pl.ds(s, first, stride=SUB), :]
    mode_one = contract_last(fold_matrix(rank, fourth), total)
    mode_one = jnp.concatenate(
        [mode_one, jnp.zeros((rank, LANES - first), jnp.float32)], axis=1
    )
    fill_slots(pay_ref, mode_one + grams)


def relay_kernel(lo, hi, in_ref, out_ref):
    value = summed_slots(in_ref)
    lane = iota(value.shape, 1)
    fill_slots(out_ref, jnp.where((lane >= lo) & (lane < hi), value * 0.125, value))


def eliminate(tiles, start, rank):
    lanes = tiles[0].shape[1]
    count = rank // SUB
    row = iota((SUB, lanes), 0)
    for b in range(count):
        cols = [
            [
                jnp.broadcast_to(tiles[t][:, start + b * SUB + c : start + b * SUB + c + 1], (SUB, lanes))
                for c in range(SUB)
            ]
            for t in range(count)
        ]
        own = tiles[b]
        piv = cols[b]
        for c in range(SUB):
            factor = piv[c]
            inverse = 1.0 / factor[c : c + 1, :]
            lead = own[c : c + 1, :] * inverse
            here = row == c
            own = jnp.where(here, lead, own - factor * lead)
            for d in range(c + 1, SUB):
                lead_d = piv[d][c : c + 1, :] * inverse
                piv[d] = jnp.where(here, lead_d, piv[d] - factor * lead_d)
        tiles[b] = own
        for t in range(count):
            if t != b:
                acc = tiles[t]
                for c in range(SUB):
                    acc = acc - cols[t][c] * own[c : c + 1, :]
                tiles[t] = acc
    return tiles


def solved(value, rank):
    lanes = value.shape[1]
    start = lanes - 2 * rank
    system = value * pltpu.roll(value, lanes - rank, 1)
    lane = iota(value.shape, 1)
    aug = jnp.where(lane < start, value, system)
    tiles = [aug[t * SUB : (t + 1) * SUB, :] for t in range(rank // SUB)]
    return jnp.concatenate(eliminate(tiles, start, rank), axis=0)


def middle_kernel(first, second, fourth, in_ref, prod_ref, new_ref, pay_ref, nx_ref, acc_ref):
    value = summed_slots(in_ref)
    rank, lanes = value.shape
    wide = fourth * rank
    rows = second * fourth
    start = lanes - 2 * rank
    answer = solved(value, rank)[:, :first]
    new_ref[...] = answer
    flat = jnp.transpose(answer)
    nx_ref[...] = jnp.concatenate([flat] * fourth, axis=1)

    def step(i, acc):
        at = pl.multiple_of(i * rows, rows)
        return acc + prod_ref[pl.ds(at, rows), :] * nx_ref[pl.ds(i, 1), :]

    acc_ref[...] = lax.fori_loop(
        0, first, step, jnp.zeros((rows, wide), jnp.float32), unroll=8
    )
    half = iota((second, wide), 1) // rank
    picked = acc_ref[pl.ds(0, second, stride=fourth), :]
    for l in range(1, fourth):
        picked = jnp.where(half == l, acc_ref[pl.ds(l, second, stride=fourth), :], picked)
    mode_two = contract_last(fold_matrix(rank, fourth), picked)
    gram_one = contract_last(answer, answer)
    head = jnp.concatenate(
        [mode_two, gram_one, jnp.zeros((rank, rank), jnp.float32)], axis=1
    )
    lane = iota(value.shape, 1)
    fill_slots(pay_ref, jnp.where(lane >= start + rank, value * 0.125, head))


def last_kernel(second, in_ref, new_ref):
    value = summed_slots(in_ref)
    new_ref[...] = solved(value, value.shape[0])[:, :second]


def exchanged(array, axis):
    return lax.all_to_all(array, axis, 0, 0, tiled=True)


def per_device(tensor, factor_two, factor_three, factor_four):
    first, second, fourth, third = tensor.shape
    rank = factor_two.shape[1]
    wide = fourth * rank
    rows = first * second * fourth
    chunks = 8
    pay = jax.ShapeDtypeStruct((8, rank, LANES), jnp.float32)
    prod, sent = pl.pallas_call(
        functools.partial(root_kernel, first, chunks),
        out_shape=(jax.ShapeDtypeStruct((rows, wide), jnp.float32), pay),
        in_specs=[pl.BlockSpec(memory_space=pl.ANY), VMEM, VMEM, VMEM],
        out_specs=(VMEM, VMEM),
        scratch_shapes=[
            pltpu.VMEM((rows, third), jnp.bfloat16),
            pltpu.VMEM((first * SUB, wide), jnp.float32),
            pltpu.SemaphoreType.DMA((chunks,)),
        ],
        compiler_params=PARAMS,
        name="root",
    )(tensor.reshape(rows, third), factor_two.T, factor_three.T, factor_four)

    def relay(array, lo, hi):
        return pl.pallas_call(
            functools.partial(relay_kernel, lo, hi),
            out_shape=pay,
            in_specs=[VMEM],
            out_specs=VMEM,
            compiler_params=PARAMS,
            name="relay",
        )(array)

    start = LANES - 2 * rank
    got = exchanged(sent, "ja")
    got = exchanged(relay(got, start, start + rank), "ka")
    new_one, sent = pl.pallas_call(
        functools.partial(middle_kernel, first, second, fourth),
        out_shape=(jax.ShapeDtypeStruct((rank, first), jnp.float32), pay),
        in_specs=[VMEM, VMEM],
        out_specs=(VMEM, VMEM),
        scratch_shapes=[
            pltpu.VMEM((first, wide), jnp.float32),
            pltpu.VMEM((second * fourth, wide), jnp.float32),
        ],
        compiler_params=PARAMS,
        name="middle",
    )(got, prod)
    got = exchanged(sent, "ia")
    got = exchanged(relay(got, start, LANES), "ka")
    new_two = pl.pallas_call(
        functools.partial(last_kernel, second),
        out_shape=jax.ShapeDtypeStruct((rank, second), jnp.float32),
        in_specs=[VMEM],
        out_specs=VMEM,
        compiler_params=PARAMS,
        name="last",
    )(got)
    return (new_one.T, new_two.T)


def solution(mesh):
    return jax.shard_map(
        per_device,
        mesh=mesh,
        in_specs=(P("ia", "ja", None, "ka"), P("ja", None), P("ka", None), P()),
        out_specs=(P("ia", None), P("ja", None)),
        check_vma=False,
    )
```

```python
import functools

import jax
import jax.numpy as jnp
from jax import lax
from jax.experimental import pallas as pl
from jax.experimental.pallas import tpu as pltpu
from jax.sharding import PartitionSpec as P

HI = lax.Precision.HIGHEST
LANES = 128
SUB = 8
PACK = 16
VMEM = pl.BlockSpec(memory_space=pltpu.VMEM)
HBM = pl.BlockSpec(memory_space=pltpu.HBM)
PARAMS = pltpu.CompilerParams(vmem_limit_bytes=24 * 1024 * 1024)


def iota(shape, dim):
    return lax.broadcasted_iota(jnp.int32, shape, dim)


def contract_last(a, b, precision=HI):
    return lax.dot_general(
        a, b, (((1,), (1,)), ((), ())), precision=precision, preferred_element_type=jnp.float32
    )


def fold_matrix(rank, fourth):
    shape = (rank, fourth * rank)
    return (iota(shape, 1) % rank == iota(shape, 0)).astype(jnp.float32)


def fill_slots(out_ref, value, at=0):
    for slot in range(out_ref.shape[0]):
        out_ref[slot, at : at + value.shape[0], :] = value


def summed_slots(ref, lo, hi):
    parts = [ref[s, lo:hi, :] for s in range(ref.shape[0])]
    while len(parts) > 1:
        parts = [a + b for a, b in zip(parts[::2], parts[1::2])]
    return parts[0]


def packed(array, groups):
    rows = array.shape[0] // groups
    return jnp.concatenate([array[g * rows : (g + 1) * rows, :] for g in range(groups)], axis=1)


def root_kernel(
    first, chunks, x_hbm, f2t_hbm, f3t_hbm, f4_hbm, prod_ref, pay_ref, rest_ref,
    x_ref, f2t_ref, f3t_ref, f4_ref, r_ref, sems,
):
    fourth, rank = f4_ref.shape
    second = f2t_ref.shape[1]
    wide = fourth * rank
    rows = second * fourth
    per = first // chunks
    span = per * rows

    def fetch(c):
        part = pl.ds(c * span, span)
        return pltpu.make_async_copy(x_hbm.at[part], x_ref.at[part], sems.at[c])

    small = [
        pltpu.make_async_copy(src, dst, sems.at[chunks + n])
        for n, (src, dst) in enumerate(((f4_hbm, f4_ref), (f3t_hbm, f3t_ref), (f2t_hbm, f2t_ref)))
    ]
    for copy in small:
        copy.start()
    for c in range(chunks):
        fetch(c).start()
    for copy in small:
        copy.wait()

    f2t = f2t_ref[...]
    f3t = f3t_ref[...]
    f4 = f4_ref[...]
    eye = iota((rank, rank), 0) == iota((rank, rank), 1)
    cols = [
        jnp.sum(jnp.where(eye, f4[l : l + 1, :], 0.0), axis=1, keepdims=True) for l in range(fourth)
    ]
    kt = jnp.concatenate([c * f3t for c in cols], axis=0).astype(jnp.bfloat16)

    spread = (iota((rows, second), 0) // fourth == iota((rows, second), 1)).astype(jnp.float32)
    weight = contract_last(spread, jnp.concatenate([f2t] * fourth, axis=0))
    keep = iota((rows, wide), 0) % fourth == iota((rows, wide), 1) // rank
    weight = jnp.where(keep, weight, 0.0).reshape(1, rows // SUB, SUB, wide)

    gram_four = sum(cols[l] * f4[l : l + 1, :] for l in range(fourth))
    groups = rank // SUB
    fill_slots(pay_ref, packed(contract_last(f2t, f2t), groups), PACK)
    rest_ref[...] = packed(contract_last(f3t, f3t) * gram_four, groups)

    for c in range(chunks):
        fetch(c).wait()
        part = contract_last(x_ref[pl.ds(c * span, span), :], kt, None)
        prod_ref[pl.ds(c * span, span), :] = part
        r_ref[pl.ds(c * per * SUB, per * SUB), :] = jnp.sum(
            part.reshape(per, rows // SUB, SUB, wide) * weight, axis=1
        ).reshape(per * SUB, wide)

    total = r_ref[pl.ds(0, first, stride=SUB), :]
    for s in range(1, SUB):
        total = total + r_ref[pl.ds(s, first, stride=SUB), :]
    fill_slots(pay_ref, packed(contract_last(fold_matrix(rank, fourth), total), 2))


def relay_kernel(in_ref, rest_ref, out_ref):
    fill_slots(out_ref, summed_slots(in_ref, 0, PACK))
    fill_slots(out_ref, rest_ref[...], PACK)


def relay_short_kernel(in_ref, out_ref):
    fill_slots(out_ref, summed_slots(in_ref, 0, PACK))


def eliminate(tiles, start, rank):
    lanes = tiles[0].shape[1]
    count = rank // SUB
    row = iota((SUB, lanes), 0)
    for b in range(count):
        cols = [
            [
                jnp.broadcast_to(tiles[t][:, start + b * SUB + c : start + b * SUB + c + 1], (SUB, lanes))
                for c in range(SUB)
            ]
            for t in range(count)
        ]
        own = tiles[b]
        piv = cols[b]
        for c in range(SUB):
            factor = piv[c]
            inverse = 1.0 / factor[c : c + 1, :]
            lead = own[c : c + 1, :] * inverse
            here = row == c
            own = jnp.where(here, lead, own - factor * lead)
            for d in range(c + 1, SUB):
                lead_d = piv[d][c : c + 1, :] * inverse
                piv[d] = jnp.where(here, lead_d, piv[d] - factor * lead_d)
        tiles[b] = own
        for t in range(count):
            if t != b:
                acc = tiles[t]
                for c in range(SUB):
                    acc = acc - cols[t][c] * own[c : c + 1, :]
                tiles[t] = acc
    return tiles


def solved(rhs, gram, rank):
    lanes = rhs.shape[1]
    start = lanes // 2
    lane = iota((SUB, lanes), 1)
    half = rhs.shape[0] // SUB
    other = pltpu.roll(rhs, start, 1)
    tiles = []
    for t in range(rank // SUB):
        own = (rhs if t < half else other)[(t % half) * SUB : (t % half + 1) * SUB, :]
        shift = (start - t * rank) % lanes
        system = pltpu.roll(gram, shift, 1) if shift else gram
        tiles.append(jnp.where(lane < start, own, system))
    return jnp.concatenate(eliminate(tiles, start, rank), axis=0)


def middle_kernel(
    first, second, fourth, two_ref, in_ref, prod_ref, new_hbm, pay_ref, rest_ref,
    new_ref, nx_ref, acc_ref, sem,
):
    rank = new_ref.shape[0]
    wide = fourth * rank
    rows = second * fourth
    rest = summed_slots(in_ref, PACK, PACK + SUB)
    gram_two = summed_slots(two_ref, PACK, PACK + SUB)
    rest_ref[...] = rest
    answer = solved(summed_slots(in_ref, 0, PACK), gram_two * rest, rank)[:, :first]
    new_ref[...] = answer
    leave = pltpu.make_async_copy(new_ref, new_hbm, sem)
    leave.start()
    flat = jnp.transpose(answer)
    nx_ref[...] = jnp.concatenate([flat] * fourth, axis=1)
    fill_slots(pay_ref, packed(contract_last(answer, answer), rank // SUB), PACK)

    def step(i, acc):
        at = pl.multiple_of(i * rows, rows)
        return acc + prod_ref[pl.ds(at, rows), :] * nx_ref[pl.ds(i, 1), :]

    acc_ref[...] = lax.fori_loop(
        0, first, step, jnp.zeros((rows, wide), jnp.float32), unroll=8
    )
    half = iota((second, wide), 1) // rank
    picked = acc_ref[pl.ds(0, second, stride=fourth), :]
    for l in range(1, fourth):
        picked = jnp.where(half == l, acc_ref[pl.ds(l, second, stride=fourth), :], picked)
    fill_slots(pay_ref, packed(contract_last(fold_matrix(rank, fourth), picked), 2))
    leave.wait()


def last_kernel(second, one_ref, rest_ref, in_ref, new_ref):
    gram_one = summed_slots(one_ref, PACK, PACK + SUB)
    rhs = summed_slots(in_ref, 0, PACK)
    new_ref[...] = solved(rhs, gram_one * rest_ref[...], new_ref.shape[0])[:, :second]


def held(array):
    return pltpu.with_memory_space_constraint(array, pltpu.HBM)


def exchanged(array, axis):
    return lax.all_to_all(array, axis, 0, 0, tiled=True)


def call(kernel, name, outs, ins, scratch=()):
    return pl.pallas_call(
        kernel,
        out_shape=tuple(jax.ShapeDtypeStruct(shape, jnp.float32) for shape, _ in outs),
        in_specs=ins,
        out_specs=tuple(spec for _, spec in outs),
        scratch_shapes=list(scratch),
        compiler_params=PARAMS,
        name=name,
    )


def per_device(tensor, factor_two, factor_three, factor_four):
    first, second, fourth, third = tensor.shape
    rank = factor_two.shape[1]
    wide = fourth * rank
    rows = first * second * fourth
    chunks = 8
    full = ((8, PACK + SUB, LANES), VMEM)
    short = ((8, PACK, LANES), VMEM)
    gram = ((SUB, LANES), VMEM)
    prod, sent, rest = call(
        functools.partial(root_kernel, first, chunks),
        "root",
        (((rows, wide), VMEM), full, gram),
        [HBM] * 4,
        (
            pltpu.VMEM((rows, third), jnp.bfloat16),
            pltpu.VMEM((rank, second), jnp.float32),
            pltpu.VMEM((rank, third), jnp.float32),
            pltpu.VMEM((fourth, rank), jnp.float32),
            pltpu.VMEM((first * SUB, wide), jnp.float32),
            pltpu.SemaphoreType.DMA((chunks + 3,)),
        ),
    )(*(held(x) for x in (tensor.reshape(rows, third), factor_two.T, factor_three.T, factor_four)))
    two = exchanged(sent, "ja")
    (sent,) = call(relay_kernel, "relay", (full,), [VMEM] * 2)(two, rest)
    got = exchanged(sent, "ka")
    new_one, sent, rest = call(
        functools.partial(middle_kernel, first, second, fourth),
        "middle",
        (((rank, first), HBM), full, gram),
        [VMEM] * 3,
        (
            pltpu.VMEM((rank, first), jnp.float32),
            pltpu.VMEM((first, wide), jnp.float32),
            pltpu.VMEM((second * fourth, wide), jnp.float32),
            pltpu.SemaphoreType.DMA,
        ),
    )(two, got, prod)
    one = exchanged(sent, "ia")
    (sent,) = call(relay_short_kernel, "relay_short", (short,), [VMEM])(one)
    got = exchanged(sent, "ka")
    (new_two,) = call(
        functools.partial(last_kernel, second), "last", (((rank, second), VMEM),), [VMEM] * 3
    )(one, rest, got)
    return (new_one.T, new_two.T)


def solution(mesh):
    return jax.shard_map(
        per_device,
        mesh=mesh,
        in_specs=(P("ia", "ja", None, "ka"), P("ja", None), P("ka", None), P()),
        out_specs=(P("ia", None), P("ja", None)),
        check_vma=False,
    )
```

```python
import functools

import jax
import jax.numpy as jnp
from jax import lax
from jax.experimental import pallas as pl
from jax.experimental.pallas import tpu as pltpu
from jax.sharding import PartitionSpec as P

HI = lax.Precision.HIGHEST
LANES = 128
SUB = 8
PACK = 16
SLOTS = 8
GROUPS = (3, 3, 2)
VMEM = pl.BlockSpec(memory_space=pltpu.VMEM)
HBM = pl.BlockSpec(memory_space=pltpu.HBM)
PARAMS = pltpu.CompilerParams(vmem_limit_bytes=24 * 1024 * 1024)


def iota(shape, dim):
    return lax.broadcasted_iota(jnp.int32, shape, dim)


def contract_last(a, b, precision=HI):
    return lax.dot_general(
        a, b, (((1,), (1,)), ((), ())), precision=precision, preferred_element_type=jnp.float32
    )


def fold_matrix(rank, fourth):
    shape = (rank, fourth * rank)
    return (iota(shape, 1) % rank == iota(shape, 0)).astype(jnp.float32)


def fill_slots(out_ref, value, at=0):
    step = out_ref.shape[0] // SLOTS
    for slot in range(SLOTS):
        out_ref[slot * step + at : slot * step + at + value.shape[0], :] = value


def summed_slots(ref, lo, hi):
    step = ref.shape[0] // SLOTS
    parts = [ref[s * step + lo : s * step + hi, :] for s in range(SLOTS)]
    while len(parts) > 1:
        parts = [a + b for a, b in zip(parts[::2], parts[1::2])]
    return parts[0]


def own_row(scratch_ref, value):
    scratch_ref[...] = value
    return scratch_ref[pl.ds(lax.axis_index("ka"), 1), :]


def row_of_each(ref, at):
    return ref[pl.ds(at, SLOTS, stride=ref.shape[0] // SLOTS), :]


def packed(array, groups):
    rows = array.shape[0] // groups
    return jnp.concatenate([array[g * rows : (g + 1) * rows, :] for g in range(groups)], axis=1)


def root_kernel(
    first, chunks, x_hbm, f2t_hbm, f3t_hbm, f4_hbm, prod_ref, pay_ref, rest_ref,
    x_ref, f2t_ref, f3t_ref, f4_ref, r_ref, g_ref, sems,
):
    fourth, rank = f4_ref.shape
    second = f2t_ref.shape[1]
    wide = fourth * rank
    rows = second * fourth
    per = first // chunks
    span = per * rows

    def fetch(c):
        part = pl.ds(c * span, span)
        return pltpu.make_async_copy(x_hbm.at[part], x_ref.at[part], sems.at[c])

    small = [
        pltpu.make_async_copy(src, dst, sems.at[chunks + n])
        for n, (src, dst) in enumerate(((f4_hbm, f4_ref), (f3t_hbm, f3t_ref), (f2t_hbm, f2t_ref)))
    ]
    for copy in small:
        copy.start()
    for c in range(chunks):
        fetch(c).start()
    for copy in small:
        copy.wait()

    f2t = f2t_ref[...]
    f3t = f3t_ref[...]
    f4 = f4_ref[...]
    eye = iota((rank, rank), 0) == iota((rank, rank), 1)
    cols = [
        jnp.sum(jnp.where(eye, f4[l : l + 1, :], 0.0), axis=1, keepdims=True) for l in range(fourth)
    ]
    kt = jnp.concatenate([c * f3t for c in cols], axis=0).astype(jnp.bfloat16)

    spread = (iota((rows, second), 0) // fourth == iota((rows, second), 1)).astype(jnp.float32)
    weight = contract_last(spread, jnp.concatenate([f2t] * fourth, axis=0))
    keep = iota((rows, wide), 0) % fourth == iota((rows, wide), 1) // rank
    weight = jnp.where(keep, weight, 0.0).reshape(1, rows // SUB, SUB, wide)

    gram_four = sum(cols[l] * f4[l : l + 1, :] for l in range(fourth))
    groups = rank // SUB
    fill_slots(pay_ref, own_row(g_ref, packed(contract_last(f2t, f2t), groups)), PACK)
    rest_ref[...] = packed(contract_last(f3t, f3t) * gram_four, groups)

    done = 0
    for group in GROUPS:
        for c in range(done, done + group):
            fetch(c).wait()
        part = contract_last(x_ref[pl.ds(done * span, group * span), :], kt, None)
        prod_ref[pl.ds(done * span, group * span), :] = part
        r_ref[pl.ds(done * per * SUB, group * per * SUB), :] = jnp.sum(
            part.reshape(group * per, rows // SUB, SUB, wide) * weight, axis=1
        ).reshape(group * per * SUB, wide)
        done += group

    total = r_ref[pl.ds(0, first, stride=SUB), :]
    for s in range(1, SUB):
        total = total + r_ref[pl.ds(s, first, stride=SUB), :]
    fill_slots(pay_ref, packed(contract_last(fold_matrix(rank, fourth), total), 2))


def relay_kernel(in_ref, rest_ref, out_ref):
    fill_slots(out_ref, summed_slots(in_ref, 0, PACK))
    fill_slots(out_ref, rest_ref[...], PACK)
    fill_slots(out_ref, summed_slots(in_ref, PACK, PACK + 1), PACK + SUB)


def relay_short_kernel(in_ref, out_ref):
    fill_slots(out_ref, summed_slots(in_ref, 0, PACK))
    fill_slots(out_ref, summed_slots(in_ref, PACK, PACK + 1), PACK)


def eliminate(tiles, start, rank):
    lanes = tiles[0].shape[1]
    count = rank // SUB
    row = iota((SUB, lanes), 0)
    for b in range(count):
        cols = [
            [
                jnp.broadcast_to(tiles[t][:, start + b * SUB + c : start + b * SUB + c + 1], (SUB, lanes))
                for c in range(SUB)
            ]
            for t in range(count)
        ]
        own = tiles[b]
        piv = cols[b]
        for c in range(SUB):
            factor = piv[c]
            inverse = 1.0 / factor[c : c + 1, :]
            lead = own[c : c + 1, :] * inverse
            here = row == c
            own = jnp.where(here, lead, own - factor * lead)
            for d in range(c + 1, SUB):
                lead_d = piv[d][c : c + 1, :] * inverse
                piv[d] = jnp.where(here, lead_d, piv[d] - factor * lead_d)
        tiles[b] = own
        for t in range(count):
            if t != b:
                acc = tiles[t]
                for c in range(SUB):
                    acc = acc - cols[t][c] * own[c : c + 1, :]
                tiles[t] = acc
    return tiles


def solved(rhs, gram, rank):
    lanes = rhs.shape[1]
    start = lanes // 2
    lane = iota((SUB, lanes), 1)
    half = rhs.shape[0] // SUB
    other = pltpu.roll(rhs, start, 1)
    tiles = []
    for t in range(rank // SUB):
        own = (rhs if t < half else other)[(t % half) * SUB : (t % half + 1) * SUB, :]
        shift = (start - t * rank) % lanes
        system = pltpu.roll(gram, shift, 1) if shift else gram
        tiles.append(jnp.where(lane < start, own, system))
    return jnp.concatenate(eliminate(tiles, start, rank), axis=0)


def middle_kernel(
    first, second, fourth, in_ref, prod_ref, new_hbm, pay_ref, rest_ref,
    new_ref, nx_ref, acc_ref, g_ref, sem,
):
    rank = new_ref.shape[0]
    wide = fourth * rank
    rows = second * fourth
    rest = summed_slots(in_ref, PACK, PACK + SUB)
    gram_two = row_of_each(in_ref, PACK + SUB)
    rest_ref[...] = rest
    answer = solved(summed_slots(in_ref, 0, PACK), gram_two * rest, rank)[:, :first]
    new_ref[...] = answer
    leave = pltpu.make_async_copy(new_ref, new_hbm, sem)
    leave.start()
    flat = jnp.transpose(answer)
    nx_ref[...] = jnp.concatenate([flat] * fourth, axis=1)
    fill_slots(pay_ref, own_row(g_ref, packed(contract_last(answer, answer), rank // SUB)), PACK)

    def step(i, acc):
        at = pl.multiple_of(i * rows, rows)
        return acc + prod_ref[pl.ds(at, rows), :] * nx_ref[pl.ds(i, 1), :]

    acc_ref[...] = lax.fori_loop(
        0, first, step, jnp.zeros((rows, wide), jnp.float32), unroll=8
    )
    half = iota((second, wide), 1) // rank
    picked = acc_ref[pl.ds(0, second, stride=fourth), :]
    for l in range(1, fourth):
        picked = jnp.where(half == l, acc_ref[pl.ds(l, second, stride=fourth), :], picked)
    fill_slots(pay_ref, packed(contract_last(fold_matrix(rank, fourth), picked), 2))
    leave.wait()


def last_kernel(second, rest_ref, in_ref, new_ref):
    gram_one = row_of_each(in_ref, PACK)
    rhs = summed_slots(in_ref, 0, PACK)
    new_ref[...] = solved(rhs, gram_one * rest_ref[...], new_ref.shape[0])[:, :second]


def held(array, space=pltpu.HBM):
    return pltpu.with_memory_space_constraint(array, space)


def exchanged(array, axis):
    rows, lanes = array.shape
    slots = array.reshape(SLOTS, rows // SLOTS, 1, lanes)
    return lax.all_to_all(slots, axis, 0, 0, tiled=True).reshape(rows, lanes)


def call(kernel, name, outs, ins, scratch=()):
    return pl.pallas_call(
        kernel,
        out_shape=tuple(jax.ShapeDtypeStruct(shape, jnp.float32) for shape, _ in outs),
        in_specs=ins,
        out_specs=tuple(spec for _, spec in outs),
        scratch_shapes=list(scratch),
        compiler_params=PARAMS,
        name=name,
    )


def per_device(tensor, factor_two, factor_three, factor_four):
    first, second, fourth, third = tensor.shape
    rank = factor_two.shape[1]
    wide = fourth * rank
    rows = first * second * fourth
    chunks = sum(GROUPS)
    narrow = ((SLOTS * (PACK + 1), LANES), VMEM)
    full = ((SLOTS * (PACK + SUB + 1), LANES), VMEM)
    gram = ((SUB, LANES), VMEM)
    prod, sent, rest = call(
        functools.partial(root_kernel, first, chunks),
        "root",
        (((rows, wide), VMEM), narrow, gram),
        [HBM] * 4,
        (
            pltpu.VMEM((rows, third), jnp.bfloat16),
            pltpu.VMEM((rank, second), jnp.float32),
            pltpu.VMEM((rank, third), jnp.float32),
            pltpu.VMEM((fourth, rank), jnp.float32),
            pltpu.VMEM((first * SUB, wide), jnp.float32),
            pltpu.VMEM((SUB, LANES), jnp.float32),
            pltpu.SemaphoreType.DMA((chunks + 3,)),
        ),
    )(*(held(x) for x in (tensor.reshape(rows, third), factor_two.T, factor_three.T, factor_four)))
    got = exchanged(sent, "ja")
    (sent,) = call(relay_kernel, "relay", (full,), [VMEM] * 2)(got, rest)
    got = exchanged(sent, "ka")
    new_one, sent, rest = call(
        functools.partial(middle_kernel, first, second, fourth),
        "middle",
        (((rank, first), HBM), narrow, gram),
        [VMEM] * 2,
        (
            pltpu.VMEM((rank, first), jnp.float32),
            pltpu.VMEM((first, wide), jnp.float32),
            pltpu.VMEM((second * fourth, wide), jnp.float32),
            pltpu.VMEM((SUB, LANES), jnp.float32),
            pltpu.SemaphoreType.DMA,
        ),
    )(got, prod)
    got = exchanged(sent, "ia")
    (sent,) = call(relay_short_kernel, "relay_short", (narrow,), [VMEM])(got)
    got = exchanged(sent, "ka")
    (new_two,) = call(
        functools.partial(last_kernel, second), "last", (((rank, second), VMEM),), [VMEM] * 2
    )(rest, got)
    return (new_one.T, new_two.T)


def solution(mesh):
    return jax.shard_map(
        per_device,
        mesh=mesh,
        in_specs=(P("ia", "ja", None, "ka"), P("ja", None), P("ka", None), P()),
        out_specs=(P("ia", None), P("ja", None)),
        check_vma=False,
    )
```

```python
import functools

import jax
import jax.numpy as jnp
from jax import lax
from jax.experimental import pallas as pl
from jax.experimental.pallas import tpu as pltpu
from jax.sharding import PartitionSpec as P

HI = lax.Precision.HIGHEST
LANES = 128
SUB = 8
PACK = 16
SLOTS = 8
VMEM = pl.BlockSpec(memory_space=pltpu.VMEM)
HBM = pl.BlockSpec(memory_space=pltpu.HBM)
PARAMS = pltpu.CompilerParams(vmem_limit_bytes=24 * 1024 * 1024)


def iota(shape, dim):
    return lax.broadcasted_iota(jnp.int32, shape, dim)


def contract_last(a, b, precision=HI):
    return lax.dot_general(
        a, b, (((1,), (1,)), ((), ())), precision=precision, preferred_element_type=jnp.float32
    )


def fold_matrix(rank, lanes):
    return (iota((rank, lanes), 1) % rank == iota((rank, lanes), 0)).astype(jnp.float32)


def fill_slots(out_ref, value, at=0):
    step = out_ref.shape[0] // SLOTS
    for slot in range(SLOTS):
        out_ref[slot * step + at : slot * step + at + value.shape[0], :] = value


def summed_slots(ref, lo, hi):
    step = ref.shape[0] // SLOTS
    parts = [ref[s * step + lo : s * step + hi, :] for s in range(SLOTS)]
    while len(parts) > 1:
        parts = [a + b for a, b in zip(parts[::2], parts[1::2])]
    return parts[0]


def own_row(scratch_ref, value):
    scratch_ref[...] = value
    return scratch_ref[pl.ds(lax.axis_index("ka"), 1), :]


def row_of_each(ref, at):
    return ref[pl.ds(at, SLOTS, stride=ref.shape[0] // SLOTS), :]


def packed(array, groups):
    rows = array.shape[0] // groups
    return jnp.concatenate([array[g * rows : (g + 1) * rows, :] for g in range(groups)], axis=1)


def root_kernel(
    first, chunks, x_hbm, f2t_hbm, f3t_hbm, f4_hbm, prod_ref, pay_ref, rest_ref,
    x_ref, f2t_ref, f3t_ref, f4_ref, r_ref, g_ref, sems,
):
    fourth, rank = f4_ref.shape
    second, third = f2t_ref.shape[1], f3t_ref.shape[1]
    wide = fourth * rank
    rows = second * fourth
    half = first // 2
    span = first * rows // chunks

    def fetch(c):
        part = pl.ds(c * span, span)
        return pltpu.make_async_copy(x_hbm.at[part], x_ref.at[part], sems.at[c])

    small = [
        pltpu.make_async_copy(src, dst, sems.at[chunks + n])
        for n, (src, dst) in enumerate(((f4_hbm, f4_ref), (f3t_hbm, f3t_ref), (f2t_hbm, f2t_ref)))
    ]
    for copy in small:
        copy.start()
    for c in range(chunks):
        fetch(c).start()
    for copy in small:
        copy.wait()

    f2t = f2t_ref[...]
    f3t = f3t_ref[...]
    f4 = f4_ref[...]
    eye = iota((rank, rank), 0) == iota((rank, rank), 1)
    cols = [
        jnp.sum(jnp.where(eye, f4[l : l + 1, :], 0.0), axis=1, keepdims=True) for l in range(fourth)
    ]
    kt = jnp.concatenate([c * f3t for c in cols], axis=0).astype(jnp.bfloat16)
    none = jnp.zeros_like(kt)
    kt = jnp.concatenate(
        [jnp.concatenate([kt, none], axis=1), jnp.concatenate([none, kt], axis=1)], axis=0
    )

    spread = (iota((rows, second), 0) // fourth == iota((rows, second), 1)).astype(jnp.float32)
    weight = contract_last(spread, jnp.concatenate([f2t] * (2 * fourth), axis=0))
    keep = iota(weight.shape, 0) % fourth == iota(weight.shape, 1) // rank % fourth
    weight = jnp.where(keep, weight, 0.0).reshape(1, rows // SUB, SUB, 2 * wide)

    gram_four = sum(cols[l] * f4[l : l + 1, :] for l in range(fourth))
    groups = rank // SUB
    fill_slots(pay_ref, own_row(g_ref, packed(contract_last(f2t, f2t), groups)), PACK)
    rest_ref[...] = packed(contract_last(f3t, f3t) * gram_four, groups)

    for c in range(chunks):
        fetch(c).wait()
    pair = jnp.concatenate([x_ref[: half * rows, :], x_ref[half * rows :, :]], axis=1)
    part = contract_last(pair, kt, None)
    prod_ref[...] = part
    r_ref[...] = jnp.sum(
        part.reshape(half, rows // SUB, SUB, 2 * wide) * weight, axis=1
    ).reshape(half * SUB, 2 * wide)

    total = r_ref[pl.ds(0, half, stride=SUB), :]
    for s in range(1, SUB):
        total = total + r_ref[pl.ds(s, half, stride=SUB), :]
    fold = fold_matrix(rank, 2 * wide)
    side = iota(fold.shape, 1) // wide
    folds = jnp.concatenate([jnp.where(side == h, fold, 0.0) for h in range(2)], axis=0)
    sums = contract_last(folds, total)
    quarters = [sums[h * rank + q : h * rank + q + PACK, :] for q in (0, PACK) for h in range(2)]
    fill_slots(pay_ref, jnp.concatenate(quarters, axis=1))


def relay_kernel(in_ref, rest_ref, out_ref):
    fill_slots(out_ref, summed_slots(in_ref, 0, PACK))
    fill_slots(out_ref, rest_ref[...], PACK)
    fill_slots(out_ref, summed_slots(in_ref, PACK, PACK + 1), PACK + SUB)


def relay_short_kernel(in_ref, out_ref):
    fill_slots(out_ref, summed_slots(in_ref, 0, PACK))
    fill_slots(out_ref, summed_slots(in_ref, PACK, PACK + 1), PACK)


def eliminate(tiles, start, rank):
    lanes = tiles[0].shape[1]
    count = rank // SUB
    row = iota((SUB, lanes), 0)
    for b in range(count):
        cols = [
            [
                jnp.broadcast_to(tiles[t][:, start + b * SUB + c : start + b * SUB + c + 1], (SUB, lanes))
                for c in range(SUB)
            ]
            for t in range(count)
        ]
        own = tiles[b]
        piv = cols[b]
        for c in range(SUB):
            factor = piv[c]
            inverse = 1.0 / factor[c : c + 1, :]
            lead = own[c : c + 1, :] * inverse
            here = row == c
            own = jnp.where(here, lead, own - factor * lead)
            for d in range(c + 1, SUB):
                lead_d = piv[d][c : c + 1, :] * inverse
                piv[d] = jnp.where(here, lead_d, piv[d] - factor * lead_d)
        tiles[b] = own
        for t in range(count):
            if t != b:
                acc = tiles[t]
                for c in range(SUB):
                    acc = acc - cols[t][c] * own[c : c + 1, :]
                tiles[t] = acc
    return tiles


def solved(rhs, gram, rank):
    lanes = rhs.shape[1]
    start = lanes // 2
    lane = iota((SUB, lanes), 1)
    half = rhs.shape[0] // SUB
    other = pltpu.roll(rhs, start, 1)
    tiles = []
    for t in range(rank // SUB):
        own = (rhs if t < half else other)[(t % half) * SUB : (t % half + 1) * SUB, :]
        shift = (start - t * rank) % lanes
        system = pltpu.roll(gram, shift, 1) if shift else gram
        tiles.append(jnp.where(lane < start, own, system))
    return jnp.concatenate(eliminate(tiles, start, rank), axis=0)


def middle_kernel(
    first, second, fourth, in_ref, prod_ref, new_hbm, pay_ref, rest_ref,
    new_ref, nx_ref, acc_ref, g_ref, sem,
):
    rank = new_ref.shape[0]
    wide = fourth * rank
    rows = second * fourth
    rest = summed_slots(in_ref, PACK, PACK + SUB)
    gram_two = row_of_each(in_ref, PACK + SUB)
    rest_ref[...] = rest
    answer = solved(summed_slots(in_ref, 0, PACK), gram_two * rest, rank)[:, :first]
    new_ref[...] = answer
    leave = pltpu.make_async_copy(new_ref, new_hbm, sem)
    leave.start()
    flat = jnp.transpose(answer)
    half = first // 2
    nx_ref[...] = jnp.concatenate([flat[:half]] * fourth + [flat[half:]] * fourth, axis=1)
    fill_slots(pay_ref, own_row(g_ref, packed(contract_last(answer, answer), rank // SUB)), PACK)

    def step(i, acc):
        at = pl.multiple_of(i * rows, rows)
        return acc + prod_ref[pl.ds(at, rows), :] * nx_ref[pl.ds(i, 1), :]

    acc_ref[...] = lax.fori_loop(
        0, half, step, jnp.zeros((rows, 2 * wide), jnp.float32), unroll=8
    )
    part = iota((second, 2 * wide), 1) // rank % fourth
    picked = acc_ref[pl.ds(0, second, stride=fourth), :]
    for l in range(1, fourth):
        picked = jnp.where(part == l, acc_ref[pl.ds(l, second, stride=fourth), :], picked)
    fill_slots(pay_ref, packed(contract_last(fold_matrix(rank, 2 * wide), picked), 2))
    leave.wait()


def last_kernel(second, rest_ref, in_ref, new_ref):
    gram_one = row_of_each(in_ref, PACK)
    rhs = summed_slots(in_ref, 0, PACK)
    new_ref[...] = solved(rhs, gram_one * rest_ref[...], new_ref.shape[0])[:, :second]


def held(array, space=pltpu.HBM):
    return pltpu.with_memory_space_constraint(array, space)


def exchanged(array, axis):
    rows, lanes = array.shape
    slots = array.reshape(SLOTS, rows // SLOTS, 1, lanes)
    return lax.all_to_all(slots, axis, 0, 0, tiled=True).reshape(rows, lanes)


def call(kernel, name, outs, ins, scratch=()):
    return pl.pallas_call(
        kernel,
        out_shape=tuple(jax.ShapeDtypeStruct(shape, jnp.float32) for shape, _ in outs),
        in_specs=ins,
        out_specs=tuple(spec for _, spec in outs),
        scratch_shapes=list(scratch),
        compiler_params=PARAMS,
        name=name,
    )


def per_device(tensor, factor_two, factor_three, factor_four):
    first, second, fourth, third = tensor.shape
    rank = factor_two.shape[1]
    wide = 2 * fourth * rank
    rows = first * second * fourth
    chunks = 8
    narrow = ((SLOTS * (PACK + 1), LANES), VMEM)
    full = ((SLOTS * (PACK + SUB + 1), LANES), VMEM)
    gram = ((SUB, LANES), VMEM)
    prod, sent, rest = call(
        functools.partial(root_kernel, first, chunks),
        "root",
        (((rows // 2, wide), VMEM), narrow, gram),
        [HBM] * 4,
        (
            pltpu.VMEM((rows, third), jnp.bfloat16),
            pltpu.VMEM((rank, second), jnp.float32),
            pltpu.VMEM((rank, third), jnp.float32),
            pltpu.VMEM((fourth, rank), jnp.float32),
            pltpu.VMEM((first // 2 * SUB, wide), jnp.float32),
            pltpu.VMEM((SUB, LANES), jnp.float32),
            pltpu.SemaphoreType.DMA((chunks + 3,)),
        ),
    )(*(held(x) for x in (tensor.reshape(rows, third), factor_two.T, factor_three.T, factor_four)))
    got = exchanged(sent, "ja")
    (sent,) = call(relay_kernel, "relay", (full,), [VMEM] * 2)(got, rest)
    got = exchanged(sent, "ka")
    new_one, sent, rest = call(
        functools.partial(middle_kernel, first, second, fourth),
        "middle",
        (((rank, first), HBM), narrow, gram),
        [VMEM] * 2,
        (
            pltpu.VMEM((rank, first), jnp.float32),
            pltpu.VMEM((first // 2, wide), jnp.float32),
            pltpu.VMEM((second * fourth, wide), jnp.float32),
            pltpu.VMEM((SUB, LANES), jnp.float32),
            pltpu.SemaphoreType.DMA,
        ),
    )(got, prod)
    got = exchanged(sent, "ia")
    (sent,) = call(relay_short_kernel, "relay_short", (narrow,), [VMEM])(got)
    got = exchanged(sent, "ka")
    (new_two,) = call(
        functools.partial(last_kernel, second), "last", (((rank, second), VMEM),), [VMEM] * 2
    )(rest, got)
    return (new_one.T, new_two.T)


def solution(mesh):
    return jax.shard_map(
        per_device,
        mesh=mesh,
        in_specs=(P("ia", "ja", None, "ka"), P("ja", None), P("ka", None), P()),
        out_specs=(P("ia", None), P("ja", None)),
        check_vma=False,
    )
```

```python
import functools

import jax
import jax.numpy as jnp
from jax import lax
from jax.experimental import pallas as pl
from jax.experimental.pallas import tpu as pltpu
from jax.sharding import Mesh
from jax.sharding import PartitionSpec as P

HI = lax.Precision.HIGHEST
LANES = 128
SUB = 8
PACK = 16
SLOTS = 8
VMEM = pl.BlockSpec(memory_space=pltpu.VMEM)
HBM = pl.BlockSpec(memory_space=pltpu.HBM)
PARAMS = pltpu.CompilerParams(vmem_limit_bytes=24 * 1024 * 1024)


def iota(shape, dim):
    return lax.broadcasted_iota(jnp.int32, shape, dim)


def contract_last(a, b, precision=HI):
    return lax.dot_general(
        a, b, (((1,), (1,)), ((), ())), precision=precision, preferred_element_type=jnp.float32
    )


def fold_matrix(rank, lanes):
    return (iota((rank, lanes), 1) % rank == iota((rank, lanes), 0)).astype(jnp.float32)


def fill_slots(out_ref, value, at=0, slots=SLOTS):
    step = out_ref.shape[0] // slots
    for slot in range(slots):
        out_ref[slot * step + at : slot * step + at + value.shape[0], :] = value


def total_of(parts):
    while len(parts) > 1:
        parts = [sum(parts[n : n + 2]) for n in range(0, len(parts), 2)]
    return parts[0]


def summed_slots(ref, lo, hi, slots=SLOTS):
    step = ref.shape[0] // slots
    return total_of([ref[s * step + lo : s * step + hi, :] for s in range(slots)])


def own_row(scratch_ref, value):
    scratch_ref[...] = value
    return scratch_ref[pl.ds(lax.axis_index("ka"), 1), :]


def row_of_each(ref, at, slots=SLOTS):
    step = ref.shape[0] // slots
    rows = [
        ref[pl.ds(first * step + at, SLOTS, stride=step), :] for first in range(0, slots, SLOTS)
    ]
    return total_of(rows)


def packed(array, groups):
    rows = array.shape[0] // groups
    return jnp.concatenate([array[g * rows : (g + 1) * rows, :] for g in range(groups)], axis=1)


def root_kernel(
    first, chunks, x_hbm, f2t_hbm, f3t_hbm, f4_hbm, prod_ref, pay_ref, rest_ref,
    x_ref, f2t_ref, f3t_ref, f4_ref, r_ref, g_ref, sems,
):
    fourth, rank = f4_ref.shape
    second, third = f2t_ref.shape[1], f3t_ref.shape[1]
    wide = fourth * rank
    rows = second * fourth
    half = first // 2
    span = first * rows // chunks

    def fetch(c):
        part = pl.ds(c * span, span)
        return pltpu.make_async_copy(x_hbm.at[part], x_ref.at[part], sems.at[c])

    small = [
        pltpu.make_async_copy(src, dst, sems.at[chunks + n])
        for n, (src, dst) in enumerate(((f4_hbm, f4_ref), (f3t_hbm, f3t_ref), (f2t_hbm, f2t_ref)))
    ]
    for copy in small:
        copy.start()
    for c in range(chunks):
        fetch(c).start()
    for copy in small:
        copy.wait()

    f2t = f2t_ref[...]
    f3t = f3t_ref[...]
    f4 = f4_ref[...]
    eye = iota((rank, rank), 0) == iota((rank, rank), 1)
    cols = [
        jnp.sum(jnp.where(eye, f4[l : l + 1, :], 0.0), axis=1, keepdims=True) for l in range(fourth)
    ]
    kt = jnp.concatenate([c * f3t for c in cols], axis=0).astype(jnp.bfloat16)
    none = jnp.zeros_like(kt)
    kt = jnp.concatenate(
        [jnp.concatenate([kt, none], axis=1), jnp.concatenate([none, kt], axis=1)], axis=0
    )

    spread = (iota((rows, second), 0) // fourth == iota((rows, second), 1)).astype(jnp.float32)
    weight = contract_last(spread, jnp.concatenate([f2t] * (2 * fourth), axis=0))
    keep = iota(weight.shape, 0) % fourth == iota(weight.shape, 1) // rank % fourth
    weight = jnp.where(keep, weight, 0.0).reshape(1, rows // SUB, SUB, 2 * wide)

    gram_four = sum(cols[l] * f4[l : l + 1, :] for l in range(fourth))
    groups = rank // SUB
    fill_slots(pay_ref, own_row(g_ref, packed(contract_last(f2t, f2t), groups)), PACK)
    rest_ref[...] = packed(contract_last(f3t, f3t) * gram_four, groups)

    for c in range(chunks):
        fetch(c).wait()
    pair = jnp.concatenate([x_ref[: half * rows, :], x_ref[half * rows :, :]], axis=1)
    part = contract_last(pair, kt, None)
    prod_ref[...] = part
    r_ref[...] = jnp.sum(
        part.reshape(half, rows // SUB, SUB, 2 * wide) * weight, axis=1
    ).reshape(half * SUB, 2 * wide)

    total = r_ref[pl.ds(0, half, stride=SUB), :]
    for s in range(1, SUB):
        total = total + r_ref[pl.ds(s, half, stride=SUB), :]
    fold = fold_matrix(rank, 2 * wide)
    side = iota(fold.shape, 1) // wide
    folds = jnp.concatenate([jnp.where(side == h, fold, 0.0) for h in range(2)], axis=0)
    sums = contract_last(folds, total)
    quarters = [sums[h * rank + q : h * rank + q + PACK, :] for q in (0, PACK) for h in range(2)]
    fill_slots(pay_ref, jnp.concatenate(quarters, axis=1))


def relay_kernel(in_ref, rest_ref, out_ref):
    fill_slots(out_ref, summed_slots(in_ref, 0, PACK))
    fill_slots(out_ref, rest_ref[...], PACK)
    fill_slots(out_ref, summed_slots(in_ref, PACK, PACK + 1), PACK + SUB)


def gather_kernel(slots, in_ref, out_ref):
    out_ref[:PACK, :] = summed_slots(in_ref, 0, PACK, slots)
    out_ref[PACK:, :] = row_of_each(in_ref, PACK, slots)


def eliminate(tiles, start, rank):
    lanes = tiles[0].shape[1]
    count = rank // SUB
    row = iota((SUB, lanes), 0)
    for b in range(count):
        cols = [
            [
                jnp.broadcast_to(tiles[t][:, start + b * SUB + c : start + b * SUB + c + 1], (SUB, lanes))
                for c in range(SUB)
            ]
            for t in range(count)
        ]
        own = tiles[b]
        piv = cols[b]
        for c in range(SUB):
            factor = piv[c]
            inverse = 1.0 / factor[c : c + 1, :]
            lead = own[c : c + 1, :] * inverse
            here = row == c
            own = jnp.where(here, lead, own - factor * lead)
            for d in range(c + 1, SUB):
                lead_d = piv[d][c : c + 1, :] * inverse
                piv[d] = jnp.where(here, lead_d, piv[d] - factor * lead_d)
        tiles[b] = own
        for t in range(count):
            if t != b:
                acc = tiles[t]
                for c in range(SUB):
                    acc = acc - cols[t][c] * own[c : c + 1, :]
                tiles[t] = acc
    return tiles


def solved(rhs, gram, rank):
    lanes = rhs.shape[1]
    start = lanes // 2
    lane = iota((SUB, lanes), 1)
    half = rhs.shape[0] // SUB
    other = pltpu.roll(rhs, start, 1)
    tiles = []
    for t in range(rank // SUB):
        own = (rhs if t < half else other)[(t % half) * SUB : (t % half + 1) * SUB, :]
        shift = (start - t * rank) % lanes
        system = pltpu.roll(gram, shift, 1) if shift else gram
        tiles.append(jnp.where(lane < start, own, system))
    return jnp.concatenate(eliminate(tiles, start, rank), axis=0)


def middle_kernel(
    first, second, fourth, slots, in_ref, prod_ref, new_hbm, pay_ref, rest_ref,
    new_ref, nx_ref, acc_ref, g_ref, sem,
):
    rank = new_ref.shape[0]
    wide = fourth * rank
    rows = second * fourth
    rest = summed_slots(in_ref, PACK, PACK + SUB)
    gram_two = row_of_each(in_ref, PACK + SUB)
    rest_ref[...] = rest
    answer = solved(summed_slots(in_ref, 0, PACK), gram_two * rest, rank)[:, :first]
    new_ref[...] = answer
    leave = pltpu.make_async_copy(new_ref, new_hbm, sem)
    leave.start()
    flat = jnp.transpose(answer)
    half = first // 2
    nx_ref[...] = jnp.concatenate([flat[:half]] * fourth + [flat[half:]] * fourth, axis=1)
    own = own_row(g_ref, packed(contract_last(answer, answer), rank // SUB))
    fill_slots(pay_ref, own, PACK, slots)

    def step(i, acc):
        at = pl.multiple_of(i * rows, rows)
        return acc + prod_ref[pl.ds(at, rows), :] * nx_ref[pl.ds(i, 1), :]

    acc_ref[...] = lax.fori_loop(
        0, half, step, jnp.zeros((rows, 2 * wide), jnp.float32), unroll=8
    )
    part = iota((second, 2 * wide), 1) // rank % fourth
    picked = acc_ref[pl.ds(0, second, stride=fourth), :]
    for l in range(1, fourth):
        picked = jnp.where(part == l, acc_ref[pl.ds(l, second, stride=fourth), :], picked)
    mode_two = contract_last(fold_matrix(rank, 2 * wide), picked)
    fill_slots(pay_ref, packed(mode_two, 2), 0, slots)
    leave.wait()


def last_kernel(second, rest_ref, own_ref, other_ref, new_ref):
    value = own_ref[...] + other_ref[...]
    gram = value[PACK:, :] * rest_ref[...]
    new_ref[...] = solved(value[:PACK, :], gram, new_ref.shape[0])[:, :second]


def held(array, space=pltpu.HBM):
    return pltpu.with_memory_space_constraint(array, space)


def exchanged(array, axes, slots=SLOTS):
    rows, lanes = array.shape
    parts = array.reshape(slots, rows // slots, 1, lanes)
    return lax.all_to_all(parts, axes, 0, 0, tiled=True).reshape(rows, lanes)


def call(kernel, name, outs, ins, scratch=()):
    return pl.pallas_call(
        kernel,
        out_shape=tuple(jax.ShapeDtypeStruct(shape, jnp.float32) for shape, _ in outs),
        in_specs=ins,
        out_specs=tuple(spec for _, spec in outs),
        scratch_shapes=list(scratch),
        compiler_params=PARAMS,
        name=name,
    )


def per_device(tensor, factor_two, factor_three, factor_four):
    first, second, fourth, third = tensor.shape
    rank = factor_two.shape[1]
    wide = 2 * fourth * rank
    rows = first * second * fourth
    chunks = 8
    narrow = ((SLOTS * (PACK + 1), LANES), VMEM)
    full = ((SLOTS * (PACK + SUB + 1), LANES), VMEM)
    gram = ((SUB, LANES), VMEM)
    prod, sent, rest = call(
        functools.partial(root_kernel, first, chunks),
        "root",
        (((rows // 2, wide), VMEM), narrow, gram),
        [HBM] * 4,
        (
            pltpu.VMEM((rows, third), jnp.bfloat16),
            pltpu.VMEM((rank, second), jnp.float32),
            pltpu.VMEM((rank, third), jnp.float32),
            pltpu.VMEM((fourth, rank), jnp.float32),
            pltpu.VMEM((first // 2 * SUB, wide), jnp.float32),
            pltpu.VMEM((SUB, LANES), jnp.float32),
            pltpu.SemaphoreType.DMA((chunks + 3,)),
        ),
    )(*(held(x) for x in (tensor.reshape(rows, third), factor_two.T, factor_three.T, factor_four)))
    got = exchanged(sent, "ja")
    (sent,) = call(relay_kernel, "relay", (full,), [VMEM] * 2)(got, rest)
    got = exchanged(sent, "ka")
    slots = lax.axis_size("x") * SLOTS
    new_one, sent, rest = call(
        functools.partial(middle_kernel, first, second, fourth, slots),
        "middle",
        (((rank, first), HBM), ((slots * (PACK + 1), LANES), VMEM), gram),
        [VMEM] * 2,
        (
            pltpu.VMEM((rank, first), jnp.float32),
            pltpu.VMEM((first // 2, wide), jnp.float32),
            pltpu.VMEM((second * fourth, wide), jnp.float32),
            pltpu.VMEM((SUB, LANES), jnp.float32),
            pltpu.SemaphoreType.DMA,
        ),
    )(got, prod)
    got = exchanged(sent, ("x", "ka"), slots)
    (own,) = call(
        functools.partial(gather_kernel, slots), "gather", (((PACK + SUB, LANES), VMEM),), [VMEM]
    )(got)
    other = lax.ppermute(own, "zh", [(0, 1), (1, 0)])
    (new_two,) = call(
        functools.partial(last_kernel, second), "last", (((rank, second), VMEM),), [VMEM] * 3
    )(rest, own, other)
    return (new_one.T, new_two.T)


def solution(mesh):
    ia, ja, ka = (mesh.shape[name] for name in ("ia", "ja", "ka"))
    parted = Mesh(mesh.devices.reshape(ia // 2, 2, ja, ka), ("x", "zh", "ja", "ka"))
    return jax.shard_map(
        per_device,
        mesh=parted,
        in_specs=(P(("x", "zh"), "ja", None, "ka"), P("ja", None), P("ka", None), P()),
        out_specs=(P(("x", "zh"), None), P("ja", None)),
        check_vma=False,
    )
```

```python
import functools

import jax
import jax.numpy as jnp
from jax import lax
from jax.experimental import pallas as pl
from jax.experimental.pallas import tpu as pltpu
from jax.sharding import Mesh
from jax.sharding import PartitionSpec as P

HI = lax.Precision.HIGHEST
LANES = 128
SUB = 8
PACK = 16
SLOTS = 8
VMEM = pl.BlockSpec(memory_space=pltpu.VMEM)
HBM = pl.BlockSpec(memory_space=pltpu.HBM)
PARAMS = pltpu.CompilerParams(vmem_limit_bytes=24 * 1024 * 1024)


def iota(shape, dim):
    return lax.broadcasted_iota(jnp.int32, shape, dim)


def contract_last(a, b, precision=HI):
    return lax.dot_general(
        a, b, (((1,), (1,)), ((), ())), precision=precision, preferred_element_type=jnp.float32
    )


def fold_matrix(rank, lanes):
    return (iota((rank, lanes), 1) % rank == iota((rank, lanes), 0)).astype(jnp.float32)


def fill_slots(out_ref, value, at=0, slots=SLOTS):
    step = out_ref.shape[0] // slots
    for slot in range(slots):
        out_ref[slot * step + at : slot * step + at + value.shape[0], :] = value


def total_of(parts):
    while len(parts) > 1:
        parts = [sum(parts[n : n + 2]) for n in range(0, len(parts), 2)]
    return parts[0]


def summed_slots(ref, lo, hi, slots=SLOTS):
    step = ref.shape[0] // slots
    return total_of([ref[s * step + lo : s * step + hi, :] for s in range(slots)])


def own_row(scratch_ref, value, lead):
    scratch_ref[...] = value
    return scratch_ref[pl.ds((lax.axis_index("ka") + SLOTS - lead % SLOTS) % SLOTS, 1), :]


def row_of_each(ref, at, slots=SLOTS):
    step = ref.shape[0] // slots
    rows = [
        ref[pl.ds(first * step + at, SLOTS, stride=step), :] for first in range(0, slots, SLOTS)
    ]
    return total_of(rows)


def packed(array, groups):
    rows = array.shape[0] // groups
    return jnp.concatenate([array[g * rows : (g + 1) * rows, :] for g in range(groups)], axis=1)


def root_kernel(
    first, chunks, x_hbm, f2t_hbm, f3t_hbm, f4_hbm, prod_ref, pay_ref, rest_ref,
    x_ref, f2t_ref, f3t_ref, f4_ref, r_ref, g_ref, sems,
):
    fourth, rank = f4_ref.shape
    second, third = f2t_ref.shape[1], f3t_ref.shape[1]
    wide = fourth * rank
    rows = second * fourth
    half = first // 2
    span = first * rows // chunks

    def fetch(c):
        part = pl.ds(c * span, span)
        return pltpu.make_async_copy(x_hbm.at[part], x_ref.at[part], sems.at[c])

    small = [
        pltpu.make_async_copy(src, dst, sems.at[chunks + n])
        for n, (src, dst) in enumerate(((f4_hbm, f4_ref), (f3t_hbm, f3t_ref), (f2t_hbm, f2t_ref)))
    ]
    for copy in small:
        copy.start()
    for c in range(chunks):
        fetch(c).start()
    for copy in small:
        copy.wait()

    f2t = f2t_ref[...]
    f3t = f3t_ref[...]
    f4 = f4_ref[...]
    eye = iota((rank, rank), 0) == iota((rank, rank), 1)
    cols = [
        jnp.sum(jnp.where(eye, f4[l : l + 1, :], 0.0), axis=1, keepdims=True) for l in range(fourth)
    ]
    kt = jnp.concatenate([c * f3t for c in cols], axis=0).astype(jnp.bfloat16)
    none = jnp.zeros_like(kt)
    kt = jnp.concatenate(
        [jnp.concatenate([kt, none], axis=1), jnp.concatenate([none, kt], axis=1)], axis=0
    )

    spread = (iota((rows, second), 0) // fourth == iota((rows, second), 1)).astype(jnp.float32)
    weight = contract_last(spread, jnp.concatenate([f2t] * (2 * fourth), axis=0))
    keep = iota(weight.shape, 0) % fourth == iota(weight.shape, 1) // rank % fourth
    weight = jnp.where(keep, weight, 0.0).reshape(1, rows // SUB, SUB, 2 * wide)

    gram_four = sum(cols[l] * f4[l : l + 1, :] for l in range(fourth))
    groups = rank // SUB
    fill_slots(pay_ref, own_row(g_ref, packed(contract_last(f2t, f2t), groups), KA_LEAD), PACK)
    rest_ref[...] = packed(contract_last(f3t, f3t) * gram_four, groups)

    for c in range(chunks):
        fetch(c).wait()
    pair = jnp.concatenate([x_ref[: half * rows, :], x_ref[half * rows :, :]], axis=1)
    part = contract_last(pair, kt, None)
    prod_ref[...] = part
    r_ref[...] = jnp.sum(
        part.reshape(half, rows // SUB, SUB, 2 * wide) * weight, axis=1
    ).reshape(half * SUB, 2 * wide)

    total = r_ref[pl.ds(0, half, stride=SUB), :]
    for s in range(1, SUB):
        total = total + r_ref[pl.ds(s, half, stride=SUB), :]
    fold = fold_matrix(rank, 2 * wide)
    side = iota(fold.shape, 1) // wide
    folds = jnp.concatenate([jnp.where(side == h, fold, 0.0) for h in range(2)], axis=0)
    sums = contract_last(folds, total)
    quarters = [sums[h * rank + q : h * rank + q + PACK, :] for q in (0, PACK) for h in range(2)]
    fill_slots(pay_ref, jnp.concatenate(quarters, axis=1))


def relay_kernel(in_ref, rest_ref, out_ref):
    fill_slots(out_ref, summed_slots(in_ref, 0, PACK))
    fill_slots(out_ref, rest_ref[...], PACK)
    fill_slots(out_ref, summed_slots(in_ref, PACK, PACK + 1), PACK + SUB)


def gather_kernel(slots, in_ref, out_ref):
    out_ref[:PACK, :] = summed_slots(in_ref, 0, PACK, slots)
    out_ref[PACK:, :] = row_of_each(in_ref, PACK, slots)


def eliminate(tiles, start, rank):
    lanes = tiles[0].shape[1]
    count = rank // SUB
    row = iota((SUB, lanes), 0)
    for b in range(count):
        cols = [
            [
                jnp.broadcast_to(tiles[t][:, start + b * SUB + c : start + b * SUB + c + 1], (SUB, lanes))
                for c in range(SUB)
            ]
            for t in range(count)
        ]
        own = tiles[b]
        piv = cols[b]
        for c in range(SUB):
            factor = piv[c]
            inverse = 1.0 / factor[c : c + 1, :]
            lead = own[c : c + 1, :] * inverse
            here = row == c
            own = jnp.where(here, lead, own - factor * lead)
            for d in range(c + 1, SUB):
                lead_d = piv[d][c : c + 1, :] * inverse
                piv[d] = jnp.where(here, lead_d, piv[d] - factor * lead_d)
        tiles[b] = own
        for t in range(count):
            if t != b:
                acc = tiles[t]
                for c in range(SUB):
                    acc = acc - cols[t][c] * own[c : c + 1, :]
                tiles[t] = acc
    return tiles


def solved(rhs, gram, rank):
    lanes = rhs.shape[1]
    start = lanes // 2
    lane = iota((SUB, lanes), 1)
    half = rhs.shape[0] // SUB
    other = pltpu.roll(rhs, start, 1)
    tiles = []
    for t in range(rank // SUB):
        own = (rhs if t < half else other)[(t % half) * SUB : (t % half + 1) * SUB, :]
        shift = (start - t * rank) % lanes
        system = pltpu.roll(gram, shift, 1) if shift else gram
        tiles.append(jnp.where(lane < start, own, system))
    return jnp.concatenate(eliminate(tiles, start, rank), axis=0)


def middle_kernel(
    first, second, fourth, slots, in_ref, prod_ref, new_hbm, pay_ref, rest_ref,
    new_ref, nx_ref, acc_ref, g_ref, sem,
):
    rank = new_ref.shape[0]
    wide = fourth * rank
    rows = second * fourth
    rest = summed_slots(in_ref, PACK, PACK + SUB)
    gram_two = row_of_each(in_ref, PACK + SUB)
    rest_ref[...] = rest
    answer = solved(summed_slots(in_ref, 0, PACK), gram_two * rest, rank)[:, :first]
    new_ref[...] = answer
    leave = pltpu.make_async_copy(new_ref, new_hbm, sem)
    leave.start()
    flat = jnp.transpose(answer)
    half = first // 2
    nx_ref[...] = jnp.concatenate([flat[:half]] * fourth + [flat[half:]] * fourth, axis=1)
    own = own_row(g_ref, packed(contract_last(answer, answer), rank // SUB), X_LEAD)
    fill_slots(pay_ref, own, PACK, slots)

    def step(i, acc):
        at = pl.multiple_of(i * rows, rows)
        return acc + prod_ref[pl.ds(at, rows), :] * nx_ref[pl.ds(i, 1), :]

    acc_ref[...] = lax.fori_loop(
        0, half, step, jnp.zeros((rows, 2 * wide), jnp.float32), unroll=8
    )
    part = iota((second, 2 * wide), 1) // rank % fourth
    picked = acc_ref[pl.ds(0, second, stride=fourth), :]
    for l in range(1, fourth):
        picked = jnp.where(part == l, acc_ref[pl.ds(l, second, stride=fourth), :], picked)
    mode_two = contract_last(fold_matrix(rank, 2 * wide), picked)
    fill_slots(pay_ref, packed(mode_two, 2), 0, slots)
    leave.wait()


def last_kernel(second, rest_ref, own_ref, other_ref, new_ref):
    value = own_ref[...] + other_ref[...]
    gram = value[PACK:, :] * rest_ref[...]
    new_ref[...] = solved(value[:PACK, :], gram, new_ref.shape[0])[:, :second]


def held(array, space=pltpu.HBM):
    return pltpu.with_memory_space_constraint(array, space)


JA_ORDER = ((7, 6, 5, 4, 3, 2, 1, 0), (7, 6, 5, 4, 3, 2, 1, 0))
KA_LEAD = 5
X_LEAD = 21


def rotated(count, lead):
    return [[(n + lead) % count for n in range(count)]]


def exchanged(array, axes, groups):
    slots = len(groups[0])
    rows, lanes = array.shape
    parts = array.reshape(slots, rows // slots, 1, lanes)
    swapped = lax.all_to_all(parts, axes, 0, 0, tiled=True, axis_index_groups=groups)
    return swapped.reshape(rows, lanes)


def call(kernel, name, outs, ins, scratch=()):
    return pl.pallas_call(
        kernel,
        out_shape=tuple(jax.ShapeDtypeStruct(shape, jnp.float32) for shape, _ in outs),
        in_specs=ins,
        out_specs=tuple(spec for _, spec in outs),
        scratch_shapes=list(scratch),
        compiler_params=PARAMS,
        name=name,
    )


def per_device(tensor, factor_two, factor_three, factor_four):
    first, second, fourth, third = tensor.shape
    rank = factor_two.shape[1]
    wide = 2 * fourth * rank
    rows = first * second * fourth
    chunks = 8
    narrow = ((SLOTS * (PACK + 1), LANES), VMEM)
    full = ((SLOTS * (PACK + SUB + 1), LANES), VMEM)
    gram = ((SUB, LANES), VMEM)
    prod, sent, rest = call(
        functools.partial(root_kernel, first, chunks),
        "root",
        (((rows // 2, wide), VMEM), narrow, gram),
        [HBM] * 4,
        (
            pltpu.VMEM((rows, third), jnp.bfloat16),
            pltpu.VMEM((rank, second), jnp.float32),
            pltpu.VMEM((rank, third), jnp.float32),
            pltpu.VMEM((fourth, rank), jnp.float32),
            pltpu.VMEM((first // 2 * SUB, wide), jnp.float32),
            pltpu.VMEM((SUB, LANES), jnp.float32),
            pltpu.SemaphoreType.DMA((chunks + 3,)),
        ),
    )(*(held(x) for x in (tensor.reshape(rows, third), factor_two.T, factor_three.T, factor_four)))
    got = exchanged(sent, ("zh", "ja"), [[h * SLOTS + j for j in JA_ORDER[h]] for h in range(2)])
    (sent,) = call(relay_kernel, "relay", (full,), [VMEM] * 2)(got, rest)
    got = exchanged(sent, "ka", rotated(SLOTS, KA_LEAD))
    slots = lax.axis_size("x") * SLOTS
    new_one, sent, rest = call(
        functools.partial(middle_kernel, first, second, fourth, slots),
        "middle",
        (((rank, first), HBM), ((slots * (PACK + 1), LANES), VMEM), gram),
        [VMEM] * 2,
        (
            pltpu.VMEM((rank, first), jnp.float32),
            pltpu.VMEM((first // 2, wide), jnp.float32),
            pltpu.VMEM((second * fourth, wide), jnp.float32),
            pltpu.VMEM((SUB, LANES), jnp.float32),
            pltpu.SemaphoreType.DMA,
        ),
    )(got, prod)
    got = exchanged(sent, ("x", "ka"), rotated(slots, X_LEAD))
    (own,) = call(
        functools.partial(gather_kernel, slots), "gather", (((PACK + SUB, LANES), VMEM),), [VMEM]
    )(got)
    other = lax.ppermute(own, "zh", [(0, 1), (1, 0)])
    (new_two,) = call(
        functools.partial(last_kernel, second), "last", (((rank, second), VMEM),), [VMEM] * 3
    )(rest, own, other)
    return (new_one.T, new_two.T)


def solution(mesh):
    ia, ja, ka = (mesh.shape[name] for name in ("ia", "ja", "ka"))
    parted = Mesh(mesh.devices.reshape(ia // 2, 2, ja, ka), ("x", "zh", "ja", "ka"))
    return jax.shard_map(
        per_device,
        mesh=parted,
        in_specs=(P(("x", "zh"), "ja", None, "ka"), P("ja", None), P("ka", None), P()),
        out_specs=(P(("x", "zh"), None), P("ja", None)),
        check_vma=False,
    )
```

```python
import functools

import jax
import jax.numpy as jnp
from jax import lax
from jax.experimental import pallas as pl
from jax.experimental.pallas import tpu as pltpu
from jax.sharding import Mesh
from jax.sharding import PartitionSpec as P

HI = lax.Precision.HIGHEST
LANES = 128
SUB = 8
PACK = 16
SLOTS = 8
VMEM = pl.BlockSpec(memory_space=pltpu.VMEM)
HBM = pl.BlockSpec(memory_space=pltpu.HBM)
PARAMS = pltpu.CompilerParams(vmem_limit_bytes=24 * 1024 * 1024)


def iota(shape, dim):
    return lax.broadcasted_iota(jnp.int32, shape, dim)


def contract_last(a, b, precision=HI):
    return lax.dot_general(
        a, b, (((1,), (1,)), ((), ())), precision=precision, preferred_element_type=jnp.float32
    )


def fold_matrix(rank, lanes):
    return (iota((rank, lanes), 1) % rank == iota((rank, lanes), 0)).astype(jnp.float32)


def fill_slots(out_ref, value, at=0):
    step = out_ref.shape[0] // SLOTS
    for slot in range(SLOTS):
        out_ref[slot * step + at : slot * step + at + value.shape[0], :] = value


def summed_slots(ref, lo, hi):
    step = ref.shape[0] // SLOTS
    parts = [ref[s * step + lo : s * step + hi, :] for s in range(SLOTS)]
    while len(parts) > 1:
        parts = [a + b for a, b in zip(parts[::2], parts[1::2])]
    return parts[0]


def own_row(scratch_ref, value, lead):
    scratch_ref[...] = value
    return scratch_ref[pl.ds((lax.axis_index("ka") + SLOTS - lead) % SLOTS, 1), :]


def row_of_each(ref, at):
    return ref[pl.ds(at, SLOTS, stride=ref.shape[0] // SLOTS), :]


def packed(array, groups):
    rows = array.shape[0] // groups
    return jnp.concatenate([array[g * rows : (g + 1) * rows, :] for g in range(groups)], axis=1)


def root_kernel(
    first, chunks, x_hbm, f2t_hbm, f3t_hbm, f4_hbm, prod_ref, pay_ref, rest_ref,
    x_ref, f2t_ref, f3t_ref, f4_ref, r_ref, g_ref, sems,
):
    fourth, rank = f4_ref.shape
    second, third = f2t_ref.shape[1], f3t_ref.shape[1]
    wide = fourth * rank
    rows = second * fourth
    half = first // 2
    span = first * rows // chunks

    def fetch(c):
        part = pl.ds(c * span, span)
        return pltpu.make_async_copy(x_hbm.at[part], x_ref.at[part], sems.at[c])

    small = [
        pltpu.make_async_copy(src, dst, sems.at[chunks + n])
        for n, (src, dst) in enumerate(((f4_hbm, f4_ref), (f3t_hbm, f3t_ref), (f2t_hbm, f2t_ref)))
    ]
    for copy in small:
        copy.start()
    for c in range(chunks):
        fetch(c).start()
    for copy in small:
        copy.wait()

    f2t = f2t_ref[...]
    f3t = f3t_ref[...]
    f4 = f4_ref[...]
    eye = iota((rank, rank), 0) == iota((rank, rank), 1)
    cols = [
        jnp.sum(jnp.where(eye, f4[l : l + 1, :], 0.0), axis=1, keepdims=True) for l in range(fourth)
    ]
    kt = jnp.concatenate([c * f3t for c in cols], axis=0).astype(jnp.bfloat16)
    none = jnp.zeros_like(kt)
    kt = jnp.concatenate(
        [jnp.concatenate([kt, none], axis=1), jnp.concatenate([none, kt], axis=1)], axis=0
    )

    spread = (iota((rows, second), 0) // fourth == iota((rows, second), 1)).astype(jnp.float32)
    weight = contract_last(spread, jnp.concatenate([f2t] * (2 * fourth), axis=0))
    keep = iota(weight.shape, 0) % fourth == iota(weight.shape, 1) // rank % fourth
    weight = jnp.where(keep, weight, 0.0).reshape(1, rows // SUB, SUB, 2 * wide)

    gram_four = sum(cols[l] * f4[l : l + 1, :] for l in range(fourth))
    groups = rank // SUB
    fill_slots(pay_ref, own_row(g_ref, packed(contract_last(f2t, f2t), groups), KA_FIRST[0]), PACK)
    rest_ref[...] = packed(contract_last(f3t, f3t) * gram_four, groups)

    for c in range(chunks):
        fetch(c).wait()
    pair = jnp.concatenate([x_ref[: half * rows, :], x_ref[half * rows :, :]], axis=1)
    part = contract_last(pair, kt, None)
    prod_ref[...] = part
    r_ref[...] = jnp.sum(
        part.reshape(half, rows // SUB, SUB, 2 * wide) * weight, axis=1
    ).reshape(half * SUB, 2 * wide)

    total = r_ref[pl.ds(0, half, stride=SUB), :]
    for s in range(1, SUB):
        total = total + r_ref[pl.ds(s, half, stride=SUB), :]
    fold = fold_matrix(rank, 2 * wide)
    side = iota(fold.shape, 1) // wide
    folds = jnp.concatenate([jnp.where(side == h, fold, 0.0) for h in range(2)], axis=0)
    sums = contract_last(folds, total)
    quarters = [sums[h * rank + q : h * rank + q + PACK, :] for q in (0, PACK) for h in range(2)]
    fill_slots(pay_ref, jnp.concatenate(quarters, axis=1))


def relay_kernel(in_ref, rest_ref, out_ref):
    fill_slots(out_ref, summed_slots(in_ref, 0, PACK))
    fill_slots(out_ref, rest_ref[...], PACK)
    fill_slots(out_ref, summed_slots(in_ref, PACK, PACK + 1), PACK + SUB)


def relay_short_kernel(in_ref, out_ref):
    fill_slots(out_ref, summed_slots(in_ref, 0, PACK))
    fill_slots(out_ref, summed_slots(in_ref, PACK, PACK + 1), PACK)


def eliminate(tiles, start, rank):
    lanes = tiles[0].shape[1]
    count = rank // SUB
    row = iota((SUB, lanes), 0)
    for b in range(count):
        cols = [
            [
                jnp.broadcast_to(tiles[t][:, start + b * SUB + c : start + b * SUB + c + 1], (SUB, lanes))
                for c in range(SUB)
            ]
            for t in range(count)
        ]
        own = tiles[b]
        piv = cols[b]
        for c in range(SUB):
            factor = piv[c]
            inverse = 1.0 / factor[c : c + 1, :]
            lead = own[c : c + 1, :] * inverse
            here = row == c
            own = jnp.where(here, lead, own - factor * lead)
            for d in range(c + 1, SUB):
                lead_d = piv[d][c : c + 1, :] * inverse
                piv[d] = jnp.where(here, lead_d, piv[d] - factor * lead_d)
        tiles[b] = own
        for t in range(count):
            if t != b:
                acc = tiles[t]
                for c in range(SUB):
                    acc = acc - cols[t][c] * own[c : c + 1, :]
                tiles[t] = acc
    return tiles


def solved(rhs, gram, rank):
    lanes = rhs.shape[1]
    start = lanes // 2
    lane = iota((SUB, lanes), 1)
    half = rhs.shape[0] // SUB
    other = pltpu.roll(rhs, start, 1)
    tiles = []
    for t in range(rank // SUB):
        own = (rhs if t < half else other)[(t % half) * SUB : (t % half + 1) * SUB, :]
        shift = (start - t * rank) % lanes
        system = pltpu.roll(gram, shift, 1) if shift else gram
        tiles.append(jnp.where(lane < start, own, system))
    return jnp.concatenate(eliminate(tiles, start, rank), axis=0)


def middle_kernel(
    first, second, fourth, in_ref, prod_ref, new_hbm, pay_ref, rest_ref,
    new_ref, nx_ref, acc_ref, g_ref, sem,
):
    rank = new_ref.shape[0]
    wide = fourth * rank
    rows = second * fourth
    rest = summed_slots(in_ref, PACK, PACK + SUB)
    gram_two = row_of_each(in_ref, PACK + SUB)
    rest_ref[...] = rest
    answer = solved(summed_slots(in_ref, 0, PACK), gram_two * rest, rank)[:, :first]
    new_ref[...] = answer
    leave = pltpu.make_async_copy(new_ref, new_hbm, sem)
    leave.start()
    flat = jnp.transpose(answer)
    half = first // 2
    nx_ref[...] = jnp.concatenate([flat[:half]] * fourth + [flat[half:]] * fourth, axis=1)
    fill_slots(pay_ref, own_row(g_ref, packed(contract_last(answer, answer), rank // SUB), KA_FIRST[1]), PACK)

    def step(i, acc):
        at = pl.multiple_of(i * rows, rows)
        return acc + prod_ref[pl.ds(at, rows), :] * nx_ref[pl.ds(i, 1), :]

    acc_ref[...] = lax.fori_loop(
        0, half, step, jnp.zeros((rows, 2 * wide), jnp.float32), unroll=8
    )
    part = iota((second, 2 * wide), 1) // rank % fourth
    picked = acc_ref[pl.ds(0, second, stride=fourth), :]
    for l in range(1, fourth):
        picked = jnp.where(part == l, acc_ref[pl.ds(l, second, stride=fourth), :], picked)
    fill_slots(pay_ref, packed(contract_last(fold_matrix(rank, 2 * wide), picked), 2))
    leave.wait()


def last_kernel(second, rest_ref, in_ref, new_ref):
    gram_one = row_of_each(in_ref, PACK)
    rhs = summed_slots(in_ref, 0, PACK)
    new_ref[...] = solved(rhs, gram_one * rest_ref[...], new_ref.shape[0])[:, :second]


def held(array, space=pltpu.HBM):
    return pltpu.with_memory_space_constraint(array, space)


JA_ORDER = ((7, 6, 5, 4, 3, 2, 1, 0), (5, 4, 6, 3, 7, 2, 1, 0))
IA_ORDER = (5, 7, 3, 1, 4, 6, 2, 0)
KA_FIRST = (5, 5)


def rotated(lead):
    return [[(n + lead) % SLOTS for n in range(SLOTS)]]


def exchanged(array, axes, groups):
    rows, lanes = array.shape
    parts = array.reshape(SLOTS, rows // SLOTS, 1, lanes)
    swapped = lax.all_to_all(parts, axes, 0, 0, tiled=True, axis_index_groups=groups)
    return swapped.reshape(rows, lanes)


def call(kernel, name, outs, ins, scratch=()):
    return pl.pallas_call(
        kernel,
        out_shape=tuple(jax.ShapeDtypeStruct(shape, jnp.float32) for shape, _ in outs),
        in_specs=ins,
        out_specs=tuple(spec for _, spec in outs),
        scratch_shapes=list(scratch),
        compiler_params=PARAMS,
        name=name,
    )


def per_device(tensor, factor_two, factor_three, factor_four):
    first, second, fourth, third = tensor.shape
    rank = factor_two.shape[1]
    wide = 2 * fourth * rank
    rows = first * second * fourth
    chunks = 8
    narrow = ((SLOTS * (PACK + 1), LANES), VMEM)
    full = ((SLOTS * (PACK + SUB + 1), LANES), VMEM)
    gram = ((SUB, LANES), VMEM)
    prod, sent, rest = call(
        functools.partial(root_kernel, first, chunks),
        "root",
        (((rows // 2, wide), VMEM), narrow, gram),
        [HBM] * 4,
        (
            pltpu.VMEM((rows, third), jnp.bfloat16),
            pltpu.VMEM((rank, second), jnp.float32),
            pltpu.VMEM((rank, third), jnp.float32),
            pltpu.VMEM((fourth, rank), jnp.float32),
            pltpu.VMEM((first // 2 * SUB, wide), jnp.float32),
            pltpu.VMEM((SUB, LANES), jnp.float32),
            pltpu.SemaphoreType.DMA((chunks + 3,)),
        ),
    )(*(held(x) for x in (tensor.reshape(rows, third), factor_two.T, factor_three.T, factor_four)))
    got = exchanged(sent, ("zh", "ja"), [[h * SLOTS + j for j in JA_ORDER[h]] for h in range(2)])
    (sent,) = call(relay_kernel, "relay", (full,), [VMEM] * 2)(got, rest)
    got = exchanged(sent, "ka", rotated(KA_FIRST[0]))
    new_one, sent, rest = call(
        functools.partial(middle_kernel, first, second, fourth),
        "middle",
        (((rank, first), HBM), narrow, gram),
        [VMEM] * 2,
        (
            pltpu.VMEM((rank, first), jnp.float32),
            pltpu.VMEM((first // 2, wide), jnp.float32),
            pltpu.VMEM((second * fourth, wide), jnp.float32),
            pltpu.VMEM((SUB, LANES), jnp.float32),
            pltpu.SemaphoreType.DMA,
        ),
    )(got, prod)
    got = exchanged(sent, ("x", "zh"), [IA_ORDER])
    (sent,) = call(relay_short_kernel, "relay_short", (narrow,), [VMEM])(got)
    got = exchanged(sent, "ka", rotated(KA_FIRST[1]))
    (new_two,) = call(
        functools.partial(last_kernel, second), "last", (((rank, second), VMEM),), [VMEM] * 2
    )(rest, got)
    return (new_one.T, new_two.T)


def solution(mesh):
    ia, ja, ka = (mesh.shape[name] for name in ("ia", "ja", "ka"))
    parted = Mesh(mesh.devices.reshape(ia // 2, 2, ja, ka), ("x", "zh", "ja", "ka"))
    return jax.shard_map(
        per_device,
        mesh=parted,
        in_specs=(P(("x", "zh"), "ja", None, "ka"), P("ja", None), P("ka", None), P()),
        out_specs=(P(("x", "zh"), None), P("ja", None)),
        check_vma=False,
    )
```

```python
import functools

import jax
import jax.numpy as jnp
from jax import lax
from jax.experimental import pallas as pl
from jax.experimental.pallas import tpu as pltpu
from jax.sharding import Mesh
from jax.sharding import PartitionSpec as P

HI = lax.Precision.HIGHEST
LANES = 128
SUB = 8
PACK = 16
PAIR = 2
SLOTS = 8
VMEM = pl.BlockSpec(memory_space=pltpu.VMEM)
HBM = pl.BlockSpec(memory_space=pltpu.HBM)
PARAMS = pltpu.CompilerParams(vmem_limit_bytes=24 * 1024 * 1024)


def iota(shape, dim):
    return lax.broadcasted_iota(jnp.int32, shape, dim)


def contract_last(a, b, precision=HI):
    return lax.dot_general(
        a, b, (((1,), (1,)), ((), ())), precision=precision, preferred_element_type=jnp.float32
    )


def pieces(array):
    out = []
    for _ in range(3):
        part = array.astype(jnp.bfloat16)
        out.append(part)
        array = array - part.astype(jnp.float32)
    return out


def packed_sums(rows, rank, keeps):
    lanes = rows.shape[1]
    halves = rank // PACK
    where = (PACK, halves * lanes)
    half, lane = iota(where, 1) // lanes, iota(where, 1) % lanes
    picks = (lane % rank == iota(where, 0) + PACK * half).astype(jnp.bfloat16)
    total = None
    for part in pieces(rows):
        blocks = []
        none = jnp.zeros_like(part)
        for h in range(halves):
            for keep in keeps:
                kept = part if keep is None else jnp.where(keep, part, none)
                blocks.append(jnp.concatenate([kept if g == h else none for g in range(halves)], axis=1))
        term = contract_last(picks, jnp.concatenate(blocks, axis=0), None)
        total = term if total is None else total + term
    return total


def fill_slots(out_ref, value, at=0):
    step = out_ref.shape[0] // SLOTS
    for slot in range(SLOTS):
        out_ref[slot * step + at : slot * step + at + value.shape[0], :] = value


def summed_slots(ref, lo, hi):
    step = ref.shape[0] // SLOTS
    parts = [ref[s * step + lo : s * step + hi, :] for s in range(SLOTS)]
    while len(parts) > 1:
        parts = [a + b for a, b in zip(parts[::2], parts[1::2])]
    return parts[0]


def own_row(scratch_ref, value, lead):
    scratch_ref[...] = value
    return scratch_ref[pl.ds((lax.axis_index("ka") + SLOTS - lead) % SLOTS, 1), :]


def row_of_each(ref, at):
    return ref[pl.ds(at, SLOTS, stride=ref.shape[0] // SLOTS), :]


def packed(array, groups):
    rows = array.shape[0] // groups
    return jnp.concatenate([array[g * rows : (g + 1) * rows, :] for g in range(groups)], axis=1)


def root_kernel(
    first, chunks, x_hbm, f2t_hbm, f3t_hbm, f4_hbm, prod_ref, pay_ref, rest_ref,
    x_ref, f2t_ref, f3t_ref, f4_ref, r_ref, g_ref, sems,
):
    fourth, rank = f4_ref.shape
    second, third = f2t_ref.shape[1], f3t_ref.shape[1]
    wide = fourth * rank
    rows = second * fourth
    half = first // 2
    span = first * rows // chunks

    def fetch(c):
        part = pl.ds(c * span, span)
        return pltpu.make_async_copy(x_hbm.at[part], x_ref.at[part], sems.at[c])

    small = [
        pltpu.make_async_copy(src, dst, sems.at[chunks + n])
        for n, (src, dst) in enumerate(((f4_hbm, f4_ref), (f3t_hbm, f3t_ref), (f2t_hbm, f2t_ref)))
    ]
    for copy in small:
        copy.start()
    for c in range(chunks):
        fetch(c).start()
    for copy in small:
        copy.wait()

    f2t = f2t_ref[...]
    f3t = f3t_ref[...]
    f4 = f4_ref[...]
    eye = iota((rank, rank), 0) == iota((rank, rank), 1)
    cols = [
        jnp.sum(jnp.where(eye, f4[l : l + 1, :], 0.0), axis=1, keepdims=True) for l in range(fourth)
    ]
    kt = jnp.concatenate([c * f3t for c in cols], axis=0).astype(jnp.bfloat16)
    none = jnp.zeros_like(kt)
    kt = jnp.concatenate(
        [jnp.concatenate([kt, none], axis=1), jnp.concatenate([none, kt], axis=1)], axis=0
    )

    spread = (iota((rows, second), 0) // fourth == iota((rows, second), 1)).astype(jnp.float32)
    weight = contract_last(spread, jnp.concatenate([f2t] * (2 * fourth), axis=0))
    keep = iota(weight.shape, 0) % fourth == iota(weight.shape, 1) // rank % fourth
    weight = jnp.where(keep, weight, 0.0).reshape(1, rows // SUB, SUB, 2 * wide)

    gram_four = sum(cols[l] * f4[l : l + 1, :] for l in range(fourth))
    groups = rank // SUB
    fill_slots(pay_ref, own_row(g_ref, packed(contract_last(f2t, f2t), groups), KA_FIRST[0]), PACK)
    rest_ref[...] = packed(contract_last(f3t, f3t) * gram_four, groups)

    for c in range(chunks):
        fetch(c).wait()
    pair = jnp.concatenate([x_ref[: half * rows, :], x_ref[half * rows :, :]], axis=1)
    part = contract_last(pair, kt, None)
    prod_ref[...] = part
    r_ref[...] = jnp.sum(
        part.reshape(half, rows // SUB, SUB, 2 * wide) * weight, axis=1
    ).reshape(half * SUB, 2 * wide)

    total = r_ref[pl.ds(0, half, stride=SUB), :]
    for s in range(1, SUB):
        total = total + r_ref[pl.ds(s, half, stride=SUB), :]
    side = iota(total.shape, 1) // wide
    fill_slots(pay_ref, packed_sums(total, rank, [side == h for h in range(2)]))


def relay_kernel(in_ref, rest_ref, out_ref):
    fill_slots(out_ref, summed_slots(in_ref, 0, PACK))
    fill_slots(out_ref, rest_ref[...], PACK)
    fill_slots(out_ref, summed_slots(in_ref, PACK, PACK + 1), PACK + SUB)


def relay_short_kernel(in_ref, out_ref):
    fill_slots(out_ref, summed_slots(in_ref, 0, PACK))
    fill_slots(out_ref, summed_slots(in_ref, PACK, PACK + 1), PACK)


def eliminate(tiles, start, rank):
    lanes = tiles[0].shape[1]
    count = rank // SUB
    row = iota((SUB, lanes), 0)
    width = PAIR * SUB
    for b in range(0, count, PAIR):
        first = start + b * SUB
        cols = [
            [
                jnp.broadcast_to(tile[:, first + c : first + c + 1], (SUB, lanes))
                for c in range(width)
            ]
            for tile in tiles
        ]
        own = tiles[b : b + PAIR]
        piv = [list(cols[b + k]) for k in range(PAIR)]
        for c in range(width):
            home, r = c // SUB, c % SUB
            here = row == r
            factors = [piv[k][c] for k in range(PAIR)]
            inverse = 1.0 / factors[home][r : r + 1, :]

            def cleared(column):
                lead = column[home][r : r + 1, :] * inverse
                rest = [column[k] - factors[k] * lead for k in range(PAIR)]
                rest[home] = jnp.where(here, lead, rest[home])
                return rest

            own = cleared(own)
            for d in range(c + 1, width):
                for k, value in enumerate(cleared([piv[k][d] for k in range(PAIR)])):
                    piv[k][d] = value
        for t in range(count):
            if b <= t < b + PAIR:
                tiles[t] = own[t - b]
            else:
                terms = [cols[t][c] * own[c // SUB][c % SUB : c % SUB + 1, :] for c in range(width)]
                while len(terms) > 1:
                    terms = [x + y for x, y in zip(terms[::2], terms[1::2])]
                tiles[t] = tiles[t] - terms[0]
    return tiles


def solved(rhs, gram, rank):
    lanes = rhs.shape[1]
    start = lanes // 2
    lane = iota((SUB, lanes), 1)
    half = rhs.shape[0] // SUB
    other = pltpu.roll(rhs, start, 1)
    tiles = []
    for t in range(rank // SUB):
        own = (rhs if t < half else other)[(t % half) * SUB : (t % half + 1) * SUB, :]
        shift = (start - t * rank) % lanes
        system = pltpu.roll(gram, shift, 1) if shift else gram
        tiles.append(jnp.where(lane < start, own, system))
    return jnp.concatenate(eliminate(tiles, start, rank), axis=0)


def middle_kernel(
    first, second, fourth, in_ref, prod_ref, new_hbm, pay_ref, rest_ref,
    new_ref, nx_ref, acc_ref, g_ref, sem,
):
    rank = new_ref.shape[0]
    wide = fourth * rank
    rows = second * fourth
    rest = summed_slots(in_ref, PACK, PACK + SUB)
    gram_two = row_of_each(in_ref, PACK + SUB)
    rest_ref[...] = rest
    answer = solved(summed_slots(in_ref, 0, PACK), gram_two * rest, rank)[:, :first]
    new_ref[...] = answer
    leave = pltpu.make_async_copy(new_ref, new_hbm, sem)
    leave.start()
    flat = jnp.transpose(answer)
    half = first // 2
    nx_ref[...] = jnp.concatenate([flat[:half]] * fourth + [flat[half:]] * fourth, axis=1)
    fill_slots(pay_ref, own_row(g_ref, packed(contract_last(answer, answer), rank // SUB), KA_FIRST[1]), PACK)

    def step(i, acc):
        at = pl.multiple_of(i * rows, rows)
        return acc + prod_ref[pl.ds(at, rows), :] * nx_ref[pl.ds(i, 1), :]

    acc_ref[...] = lax.fori_loop(
        0, half, step, jnp.zeros((rows, 2 * wide), jnp.float32), unroll=8
    )
    part = iota((second, 2 * wide), 1) // rank % fourth
    picked = acc_ref[pl.ds(0, second, stride=fourth), :]
    for l in range(1, fourth):
        picked = jnp.where(part == l, acc_ref[pl.ds(l, second, stride=fourth), :], picked)
    fill_slots(pay_ref, packed_sums(picked, rank, [None]))
    leave.wait()


def last_kernel(second, rest_ref, in_ref, new_ref):
    gram_one = row_of_each(in_ref, PACK)
    rhs = summed_slots(in_ref, 0, PACK)
    new_ref[...] = solved(rhs, gram_one * rest_ref[...], new_ref.shape[0])[:, :second]


def held(array, space=pltpu.HBM):
    return pltpu.with_memory_space_constraint(array, space)


JA_ORDER = ((7, 6, 5, 4, 3, 2, 1, 0), (5, 4, 6, 3, 7, 2, 1, 0))
IA_ORDER = (5, 4, 6, 2, 0, 7, 3, 1)
KA_FIRST = (5, 5)


def rotated(lead):
    return [[(n + lead) % SLOTS for n in range(SLOTS)]]


def exchanged(array, axes, groups):
    rows, lanes = array.shape
    parts = array.reshape(SLOTS, rows // SLOTS, 1, lanes)
    swapped = lax.all_to_all(parts, axes, 0, 0, tiled=True, axis_index_groups=groups)
    return swapped.reshape(rows, lanes)


def call(kernel, name, outs, ins, scratch=()):
    return pl.pallas_call(
        kernel,
        out_shape=tuple(jax.ShapeDtypeStruct(shape, jnp.float32) for shape, _ in outs),
        in_specs=ins,
        out_specs=tuple(spec for _, spec in outs),
        scratch_shapes=list(scratch),
        compiler_params=PARAMS,
        name=name,
    )


def per_device(tensor, factor_two, factor_three, factor_four):
    first, second, fourth, third = tensor.shape
    rank = factor_two.shape[1]
    wide = 2 * fourth * rank
    rows = first * second * fourth
    chunks = 8
    narrow = ((SLOTS * (PACK + 1), LANES), VMEM)
    full = ((SLOTS * (PACK + SUB + 1), LANES), VMEM)
    gram = ((SUB, LANES), VMEM)
    prod, sent, rest = call(
        functools.partial(root_kernel, first, chunks),
        "root",
        (((rows // 2, wide), VMEM), narrow, gram),
        [HBM] * 4,
        (
            pltpu.VMEM((rows, third), jnp.bfloat16),
            pltpu.VMEM((rank, second), jnp.float32),
            pltpu.VMEM((rank, third), jnp.float32),
            pltpu.VMEM((fourth, rank), jnp.float32),
            pltpu.VMEM((first // 2 * SUB, wide), jnp.float32),
            pltpu.VMEM((SUB, LANES), jnp.float32),
            pltpu.SemaphoreType.DMA((chunks + 3,)),
        ),
    )(*(held(x) for x in (tensor.reshape(rows, third), factor_two.T, factor_three.T, factor_four)))
    got = exchanged(sent, ("zh", "ja"), [[h * SLOTS + j for j in JA_ORDER[h]] for h in range(2)])
    (sent,) = call(relay_kernel, "relay", (full,), [VMEM] * 2)(got, rest)
    got = exchanged(sent, "ka", rotated(KA_FIRST[0]))
    new_one, sent, rest = call(
        functools.partial(middle_kernel, first, second, fourth),
        "middle",
        (((rank, first), HBM), narrow, gram),
        [VMEM] * 2,
        (
            pltpu.VMEM((rank, first), jnp.float32),
            pltpu.VMEM((first // 2, wide), jnp.float32),
            pltpu.VMEM((second * fourth, wide), jnp.float32),
            pltpu.VMEM((SUB, LANES), jnp.float32),
            pltpu.SemaphoreType.DMA,
        ),
    )(got, prod)
    got = exchanged(sent, ("x", "zh"), [IA_ORDER])
    (sent,) = call(relay_short_kernel, "relay_short", (narrow,), [VMEM])(got)
    got = exchanged(sent, "ka", rotated(KA_FIRST[1]))
    (new_two,) = call(
        functools.partial(last_kernel, second), "last", (((rank, second), VMEM),), [VMEM] * 2
    )(rest, got)
    return (new_one.T, new_two.T)


def solution(mesh):
    ia, ja, ka = (mesh.shape[name] for name in ("ia", "ja", "ka"))
    parted = Mesh(mesh.devices.reshape(ia // 2, 2, ja, ka), ("x", "zh", "ja", "ka"))
    return jax.shard_map(
        per_device,
        mesh=parted,
        in_specs=(P(("x", "zh"), "ja", None, "ka"), P("ja", None), P("ka", None), P()),
        out_specs=(P(("x", "zh"), None), P("ja", None)),
        check_vma=False,
    )
```

```python
import functools

import jax
import jax.numpy as jnp
from jax import lax
from jax.experimental import pallas as pl
from jax.experimental.pallas import tpu as pltpu
from jax.sharding import Mesh
from jax.sharding import PartitionSpec as P

HI = lax.Precision.HIGHEST
LANES = 128
SUB = 8
PACK = 16
PAIR = 2
SLOTS = 8
VMEM = pl.BlockSpec(memory_space=pltpu.VMEM)
HBM = pl.BlockSpec(memory_space=pltpu.HBM)
PARAMS = pltpu.CompilerParams(vmem_limit_bytes=24 * 1024 * 1024)


def iota(shape, dim):
    return lax.broadcasted_iota(jnp.int32, shape, dim)


def contract_last(a, b, precision=HI):
    return lax.dot_general(
        a, b, (((1,), (1,)), ((), ())), precision=precision, preferred_element_type=jnp.float32
    )


def pieces(array):
    out = []
    for _ in range(3):
        part = array.astype(jnp.bfloat16)
        out.append(part)
        array = array - part.astype(jnp.float32)
    return out


def packed_sums(rows, rank, keeps):
    lanes = rows.shape[1]
    halves = rank // PACK
    where = (PACK, halves * lanes)
    half, lane = iota(where, 1) // lanes, iota(where, 1) % lanes
    picks = (lane % rank == iota(where, 0) + PACK * half).astype(jnp.bfloat16)
    total = None
    for part in pieces(rows):
        blocks = []
        none = jnp.zeros_like(part)
        for h in range(halves):
            for keep in keeps:
                kept = part if keep is None else jnp.where(keep, part, none)
                blocks.append(jnp.concatenate([kept if g == h else none for g in range(halves)], axis=1))
        term = contract_last(picks, jnp.concatenate(blocks, axis=0), None)
        total = term if total is None else total + term
    return total


def fill_slots(out_ref, value, at=0):
    step = out_ref.shape[0] // SLOTS
    for slot in range(SLOTS):
        out_ref[slot * step + at : slot * step + at + value.shape[0], :] = value


def summed_slots(ref, lo, hi):
    step = ref.shape[0] // SLOTS
    parts = [ref[s * step + lo : s * step + hi, :] for s in range(SLOTS)]
    while len(parts) > 1:
        parts = [a + b for a, b in zip(parts[::2], parts[1::2])]
    return parts[0]


def own_row(scratch_ref, value, lead):
    scratch_ref[...] = value
    return scratch_ref[pl.ds((lax.axis_index("ka") + SLOTS - lead) % SLOTS, 1), :]


def row_of_each(ref, at):
    return ref[pl.ds(at, SLOTS, stride=ref.shape[0] // SLOTS), :]


def packed(array, groups):
    rows = array.shape[0] // groups
    return jnp.concatenate([array[g * rows : (g + 1) * rows, :] for g in range(groups)], axis=1)


def root_kernel(
    first, chunks, x_hbm, f2t_hbm, f3t_hbm, f4_hbm, prod_ref, pay_ref, rest_ref,
    x_ref, f2t_ref, f3t_ref, f4_ref, r_ref, g_ref, sems,
):
    fourth, rank = f4_ref.shape
    second, third = f2t_ref.shape[1], f3t_ref.shape[1]
    wide = fourth * rank
    rows = second * fourth
    half = first // 2
    span = first * rows // chunks

    def fetch(c):
        part = pl.ds(c * span, span)
        return pltpu.make_async_copy(x_hbm.at[part], x_ref.at[part], sems.at[c])

    small = [
        pltpu.make_async_copy(src, dst, sems.at[chunks + n])
        for n, (src, dst) in enumerate(((f4_hbm, f4_ref), (f3t_hbm, f3t_ref), (f2t_hbm, f2t_ref)))
    ]
    for copy in small:
        copy.start()
    for c in range(chunks):
        fetch(c).start()
    for copy in small:
        copy.wait()

    f2t = f2t_ref[...]
    f3t = f3t_ref[...]
    f4 = f4_ref[...]
    eye = iota((rank, rank), 0) == iota((rank, rank), 1)
    cols = [
        jnp.sum(jnp.where(eye, f4[l : l + 1, :], 0.0), axis=1, keepdims=True) for l in range(fourth)
    ]
    kt = jnp.concatenate([c * f3t for c in cols], axis=0).astype(jnp.bfloat16)
    none = jnp.zeros_like(kt)
    kt = jnp.concatenate(
        [jnp.concatenate([kt, none], axis=1), jnp.concatenate([none, kt], axis=1)], axis=0
    )

    spread = (iota((rows, second), 0) // fourth == iota((rows, second), 1)).astype(jnp.float32)
    weight = contract_last(spread, jnp.concatenate([f2t] * (2 * fourth), axis=0))
    keep = iota(weight.shape, 0) % fourth == iota(weight.shape, 1) // rank % fourth
    weight = jnp.where(keep, weight, 0.0).reshape(1, rows // SUB, SUB, 2 * wide)

    gram_four = sum(cols[l] * f4[l : l + 1, :] for l in range(fourth))
    groups = rank // SUB
    fill_slots(pay_ref, own_row(g_ref, packed(contract_last(f2t, f2t), groups), KA_FIRST[0]), PACK)
    rest_ref[...] = packed(contract_last(f3t, f3t) * gram_four, groups)

    for c in range(chunks):
        fetch(c).wait()
    pair = jnp.concatenate([x_ref[: half * rows, :], x_ref[half * rows :, :]], axis=1)
    part = contract_last(pair, kt, None)
    prod_ref[...] = part
    r_ref[...] = jnp.sum(
        part.reshape(half, rows // SUB, SUB, 2 * wide) * weight, axis=1
    ).reshape(half * SUB, 2 * wide)

    total = r_ref[pl.ds(0, half, stride=SUB), :]
    for s in range(1, SUB):
        total = total + r_ref[pl.ds(s, half, stride=SUB), :]
    side = iota(total.shape, 1) // wide
    fill_slots(pay_ref, packed_sums(total, rank, [side == h for h in range(2)]))


def relay_kernel(in_ref, rest_ref, out_ref):
    fill_slots(out_ref, summed_slots(in_ref, 0, PACK))
    fill_slots(out_ref, rest_ref[...], PACK)
    fill_slots(out_ref, summed_slots(in_ref, PACK, PACK + 1), PACK + SUB)


def relay_short_kernel(in_ref, out_ref):
    fill_slots(out_ref, summed_slots(in_ref, 0, PACK))
    fill_slots(out_ref, summed_slots(in_ref, PACK, PACK + 1), PACK)


def eliminate(tiles, start, rank):
    lanes = tiles[0].shape[1]
    count = rank // SUB
    row = iota((SUB, lanes), 0)
    width = PAIR * SUB
    for b in range(0, count, PAIR):
        first = start + b * SUB
        cols = [
            [
                jnp.broadcast_to(tile[:, first + c : first + c + 1], (SUB, lanes))
                for c in range(width)
            ]
            for tile in tiles
        ]
        own = tiles[b : b + PAIR]
        piv = [list(cols[b + k]) for k in range(PAIR)]
        for c in range(width):
            home, r = c // SUB, c % SUB
            here = row == r
            factors = [piv[k][c] for k in range(PAIR)]
            inverse = 1.0 / factors[home][r : r + 1, :]

            def cleared(column):
                lead = column[home][r : r + 1, :] * inverse
                rest = [column[k] - factors[k] * lead for k in range(PAIR)]
                rest[home] = jnp.where(here, lead, rest[home])
                return rest

            own = cleared(own)
            for d in range(c + 1, width):
                for k, value in enumerate(cleared([piv[k][d] for k in range(PAIR)])):
                    piv[k][d] = value
        for t in range(count):
            if b <= t < b + PAIR:
                tiles[t] = own[t - b]
            else:
                terms = [cols[t][c] * own[c // SUB][c % SUB : c % SUB + 1, :] for c in range(width)]
                while len(terms) > 1:
                    terms = [x + y for x, y in zip(terms[::2], terms[1::2])]
                tiles[t] = tiles[t] - terms[0]
    return tiles


def solved(rhs, gram, rank):
    lanes = rhs.shape[1]
    start = lanes // 2
    lane = iota((SUB, lanes), 1)
    half = rhs.shape[0] // SUB
    other = pltpu.roll(rhs, start, 1)
    tiles = []
    for t in range(rank // SUB):
        own = (rhs if t < half else other)[(t % half) * SUB : (t % half + 1) * SUB, :]
        shift = (start - t * rank) % lanes
        system = pltpu.roll(gram, shift, 1) if shift else gram
        tiles.append(jnp.where(lane < start, own, system))
    return jnp.concatenate(eliminate(tiles, start, rank), axis=0)


def middle_kernel(
    first, second, fourth, in_ref, prod_ref, new_hbm, pay_ref, rest_ref,
    new_ref, nx_ref, acc_ref, g_ref, sem,
):
    rank = new_ref.shape[0]
    wide = fourth * rank
    rows = second * fourth
    rest = summed_slots(in_ref, PACK, PACK + SUB)
    gram_two = row_of_each(in_ref, PACK + SUB)
    rest_ref[...] = rest
    answer = solved(summed_slots(in_ref, 0, PACK), gram_two * rest, rank)[:, :first]
    new_ref[...] = answer
    leave = pltpu.make_async_copy(new_ref, new_hbm, sem)
    leave.start()
    flat = jnp.transpose(answer)
    half = first // 2
    nx_ref[...] = jnp.concatenate([flat[:half]] * fourth + [flat[half:]] * fourth, axis=1)
    fill_slots(pay_ref, own_row(g_ref, packed(contract_last(answer, answer), rank // SUB), KA_FIRST[1]), PACK)

    def step(i, acc):
        at = pl.multiple_of(i * rows, rows)
        return acc + prod_ref[pl.ds(at, rows), :] * nx_ref[pl.ds(i, 1), :]

    acc_ref[...] = lax.fori_loop(
        0, half, step, jnp.zeros((rows, 2 * wide), jnp.float32), unroll=16
    )
    part = iota((second, 2 * wide), 1) // rank % fourth
    picked = acc_ref[pl.ds(0, second, stride=fourth), :]
    for l in range(1, fourth):
        picked = jnp.where(part == l, acc_ref[pl.ds(l, second, stride=fourth), :], picked)
    fill_slots(pay_ref, packed_sums(picked, rank, [None]))
    leave.wait()


def last_kernel(second, rest_ref, in_ref, new_ref):
    gram_one = row_of_each(in_ref, PACK)
    rhs = summed_slots(in_ref, 0, PACK)
    new_ref[...] = solved(rhs, gram_one * rest_ref[...], new_ref.shape[0])[:, :second]


def held(array, space=pltpu.HBM):
    return pltpu.with_memory_space_constraint(array, space)


JA_ORDER = ((7, 6, 5, 4, 3, 2, 1, 0), (5, 4, 6, 3, 7, 2, 1, 0))
IA_ORDER = (5, 4, 6, 2, 0, 7, 3, 1)
KA_FIRST = (5, 5)


def rotated(lead):
    return [[(n + lead) % SLOTS for n in range(SLOTS)]]


def exchanged(array, axes, groups):
    rows, lanes = array.shape
    parts = array.reshape(SLOTS, rows // SLOTS, 1, lanes)
    swapped = lax.all_to_all(parts, axes, 0, 0, tiled=True, axis_index_groups=groups)
    return swapped.reshape(rows, lanes)


def call(kernel, name, outs, ins, scratch=()):
    return pl.pallas_call(
        kernel,
        out_shape=tuple(jax.ShapeDtypeStruct(shape, jnp.float32) for shape, _ in outs),
        in_specs=ins,
        out_specs=tuple(spec for _, spec in outs),
        scratch_shapes=list(scratch),
        compiler_params=PARAMS,
        name=name,
    )


def per_device(tensor, factor_two, factor_three, factor_four):
    first, second, fourth, third = tensor.shape
    rank = factor_two.shape[1]
    wide = 2 * fourth * rank
    rows = first * second * fourth
    chunks = 4
    narrow = ((SLOTS * (PACK + 1), LANES), VMEM)
    full = ((SLOTS * (PACK + SUB + 1), LANES), VMEM)
    gram = ((SUB, LANES), VMEM)
    prod, sent, rest = call(
        functools.partial(root_kernel, first, chunks),
        "root",
        (((rows // 2, wide), VMEM), narrow, gram),
        [HBM] * 4,
        (
            pltpu.VMEM((rows, third), jnp.bfloat16),
            pltpu.VMEM((rank, second), jnp.float32),
            pltpu.VMEM((rank, third), jnp.float32),
            pltpu.VMEM((fourth, rank), jnp.float32),
            pltpu.VMEM((first // 2 * SUB, wide), jnp.float32),
            pltpu.VMEM((SUB, LANES), jnp.float32),
            pltpu.SemaphoreType.DMA((chunks + 3,)),
        ),
    )(*(held(x) for x in (tensor.reshape(rows, third), factor_two.T, factor_three.T, factor_four)))
    got = exchanged(sent, ("zh", "ja"), [[h * SLOTS + j for j in JA_ORDER[h]] for h in range(2)])
    (sent,) = call(relay_kernel, "relay", (full,), [VMEM] * 2)(got, rest)
    got = exchanged(sent, "ka", rotated(KA_FIRST[0]))
    new_one, sent, rest = call(
        functools.partial(middle_kernel, first, second, fourth),
        "middle",
        (((rank, first), HBM), narrow, gram),
        [VMEM] * 2,
        (
            pltpu.VMEM((rank, first), jnp.float32),
            pltpu.VMEM((first // 2, wide), jnp.float32),
            pltpu.VMEM((second * fourth, wide), jnp.float32),
            pltpu.VMEM((SUB, LANES), jnp.float32),
            pltpu.SemaphoreType.DMA,
        ),
    )(got, prod)
    got = exchanged(sent, ("x", "zh"), [IA_ORDER])
    (sent,) = call(relay_short_kernel, "relay_short", (narrow,), [VMEM])(got)
    got = exchanged(sent, "ka", rotated(KA_FIRST[1]))
    (new_two,) = call(
        functools.partial(last_kernel, second), "last", (((rank, second), VMEM),), [VMEM] * 2
    )(rest, got)
    return (new_one.T, new_two.T)


def solution(mesh):
    ia, ja, ka = (mesh.shape[name] for name in ("ia", "ja", "ka"))
    parted = Mesh(mesh.devices.reshape(ia // 2, 2, ja, ka), ("x", "zh", "ja", "ka"))
    return jax.shard_map(
        per_device,
        mesh=parted,
        in_specs=(P(("x", "zh"), "ja", None, "ka"), P("ja", None), P("ka", None), P()),
        out_specs=(P(("x", "zh"), None), P("ja", None)),
        check_vma=False,
    )
```
